32 devices in a mesh: section: 2 (over x), expert: 8 (over z, y), replica: 2 (over core).
Axes of the slice: x: 2, y: 2, z: 4, core: 2. Of those that a mesh axis runs over, the one named last changes fastest.
Arguments:
- token_grads: bfloat16 [2, 512, 3584], P('section', 'expert', 'replica'), may hold values from -6 to 6
- routing: int32 [2, 512, 1], P('section', 'expert'), may hold values from 0 to 1; in each aligned block of 64 rows (0 to 63, 64 to 127, ..., all dimensions but the last counted through in order) at most 34 rows name the same one
- gate_weights: float32 [2, 512, 1], P('section', 'expert'), may hold values from 0.1 to 1
- layer_inputs: bfloat16 [2, 512, 3584], P('section', 'expert', 'replica'), may hold values from -6 to 6
- w_gate: bfloat16 [2, 3584, 2048], P('section', 'replica', 'expert'), may hold values from -0.09375 to 0.09375
- w_up: bfloat16 [2, 3584, 2048], P('section', 'replica', 'expert'), may hold values from -0.09375 to 0.09375
- w_down: bfloat16 [2, 3584, 2048], P('section', 'replica', 'expert'), may hold values from -0.09375 to 0.09375
Outputs:
- upstream: bfloat16 [2, 512, 3584], P('section', 'expert', 'replica')
- grad_gate: bfloat16 [2, 3584, 2048], P('section', 'replica', 'expert')
- grad_up: bfloat16 [2, 3584, 2048], P('section', 'replica', 'expert')
- grad_down: bfloat16 [2, 3584, 2048], P('section', 'replica', 'expert')
The draws below stay inside these ranges and needn't reach their ends.
Inputs may be any that keep to these rules, and one draw needn't show every extreme that they name: `routing`: each token names 1 different experts. Among the 64 tokens of one group no expert is named more than 34 times, and in every draw some group names some expert exactly 34 times.
All inputs are finite; a program needn't handle non-finite values.
Results may differ from the reference program's by a relative error of at most 0.0064.
Values may be sent and summed in bfloat16 or wider, within the bound.
No kernel may reach another device: no remote copies, remote signals or barrier semaphores. Data moves between devices by JAX's collectives and lax.ppermute only.
A program may use at most 64 MiB of HBM per device.

```python
import math
import jax
import jax.numpy as jnp
import numpy as np
from jax import lax

D = 3584
FFW = 1024
SHARES = 4
EXPERTS = 2
TOP = 1
TOK_DEV = 64
CAP = 34
TOKENS = 512
N_SECTION = 2
N_EXPERT = 8


def shard_levels(own_key, dims, pieces, least, largest):
    loudness = 1.0
    for axis_at, parts in pieces:
        heights = jax.random.uniform(jax.random.fold_in(jax.random.fold_in(own_key, 6), axis_at), (parts,), jnp.float32, least / len(pieces), largest / len(pieces))
        loudness = loudness * jnp.repeat(jnp.exp(heights), dims[axis_at] // parts).reshape((-1,) + (1,) * (len(dims) - 1 - axis_at))
    return loudness


def routed_block(rng, own, number, rows, count, top, most, slope):
    ranking = jax.random.permutation(rng, count)
    heavy_load, ordinary = shares(count, rows * top, most, slope, True), shares(count, rows * top, most, slope, False)
    places = jnp.arange(count)

    def named(lengths, turn):
        used = int((lengths > 0).sum())
        fixed = max(1, used // 4)
        moved = fixed + (places - fixed + turn * (used - fixed)) % max(1, count - fixed)
        return jnp.zeros((count,), jnp.int32).at[ranking[jnp.where(places < fixed, places, moved)]].set(jnp.asarray(lengths, jnp.int32))

    lengths = jnp.where(number % 4 == 0, named(heavy_load, number // 4), named(ordinary, number - number // 4 - 1))
    mixed = jax.random.permutation(jax.random.fold_in(own, 3), count)
    donor, taker = mixed[0:count // 2 * 2:2], mixed[1:count // 2 * 2:2]
    room = jnp.minimum(lengths[donor] - 1, most - lengths[taker]) // 2
    room = jnp.where((donor == ranking[0]) | (taker == ranking[0]) | (lengths[taker] == 0), 0, jnp.maximum(room, 0))
    moved = jax.random.randint(jax.random.fold_in(own, 4), (count // 2,), 0, 1 << 20) % (room + 1)
    lengths = lengths.at[donor].add(-moved).at[taker].add(moved)
    items = jnp.searchsorted(jnp.cumsum(lengths), jnp.arange(rows * top), side="right").astype(jnp.int32)
    grid = items.reshape(top, rows).T
    grid = grid[jax.random.permutation(jax.random.fold_in(own, 1), rows)]
    turn = jax.random.randint(jax.random.fold_in(own, 2), (rows, 1), 0, top)
    return jnp.take_along_axis(grid, (jnp.arange(top)[None, :] + turn) % top, axis=1)


def shares(number_of, total, reach, skew, full):
    weights = [(1 << 20) // math.isqrt(standing ** skew) + 1 for standing in range(1, number_of + 1)]
    largest = reach if full else min(reach, max(-(-total // number_of), total * weights[0] // sum(weights)))
    least = 1 if total - largest >= number_of - 1 else 0
    holding, rest = [largest] + [least] * (number_of - 1), total - largest - least * (number_of - 1)
    while rest > 0:
        free = [i for i in range(1, number_of) if holding[i] < largest] or [i for i in range(1, number_of) if holding[i] < reach]
        whole, left = sum([weights[i] for i in free]), rest
        for i in free:
            more = min(reach - holding[i], max(1, left * weights[i] // whole), rest)
            holding[i] = holding[i] + more
            rest = rest - more
    return np.array(holding)


def normal_values(own_key, dims, deviation, limit, split=(), kind=jnp.bfloat16):
    drawn = jax.random.normal(own_key, dims, jnp.float32) * deviation
    if len(split) > 0:
        drawn = shard_levels(own_key, dims, split, -0.22, 0.18) * drawn
    return jnp.clip(drawn, min=-limit, max=limit).astype(kind)


def setup_inputs(seed: int = 0) -> dict:
    streams_of = jax.random.split(jax.random.key(seed), 8)
    token_grads = normal_values(streams_of[0], (N_SECTION, TOKENS, D), 1.0, 6.0, ((0, 2), (1, 8), (2, 2)))
    routing_keys = jax.random.split(jax.random.fold_in(streams_of[1], 1), N_SECTION * TOKENS // TOK_DEV)
    routing_turns = jax.random.permutation(jax.random.fold_in(streams_of[1], 3), N_SECTION * TOKENS // TOK_DEV)
    routing = jax.vmap(lambda own, number: routed_block(jax.random.fold_in(streams_of[1], 2), own, number, TOK_DEV, EXPERTS, TOP, CAP, 2))(routing_keys, routing_turns).reshape((N_SECTION, TOKENS, TOP))
    gate_weights = jnp.clip(jnp.exp(math.log(1.0) - 2.3025851 * jax.random.uniform(streams_of[2], (N_SECTION, TOKENS, TOP), jnp.float32) ** shard_levels(streams_of[2], (N_SECTION, TOKENS, TOP), ((0, 2), (1, 8)), -0.2, 0.2)), 0.1, 1.0)
    layer_inputs = normal_values(streams_of[3], (N_SECTION, TOKENS, D), 1.0, 6.0, ((0, 2), (1, 8), (2, 2)))
    w_gate = normal_values(streams_of[4], (N_SECTION, D, EXPERTS * FFW), D ** -0.5, 0.09375, ((0, 2), (1, 2), (2, 8)))
    w_up = normal_values(streams_of[5], (N_SECTION, D, EXPERTS * FFW), D ** -0.5, 0.09375, ((0, 2), (1, 2), (2, 8)))
    w_down = normal_values(streams_of[6], (N_SECTION, D, EXPERTS * FFW), D ** -0.5, 0.09375, ((0, 2), (1, 2), (2, 8)))
    return {"token_grads": token_grads, "routing": routing, "gate_weights": gate_weights, "layer_inputs": layer_inputs, "w_gate": w_gate, "w_up": w_up, "w_down": w_down}


def slot_index(routes, n_experts, capacity):
    flat_route = routes.reshape(-1).astype(jnp.int32)
    one_hot = (flat_route[:, None] == jnp.arange(n_experts, dtype=jnp.int32)[None, :]).astype(jnp.int32)
    before = jnp.cumsum(one_hot, axis=0) - one_hot
    rank_in = jnp.sum(before * one_hot, axis=1)
    return (flat_route * capacity + rank_in).astype(jnp.int32)


def dispatch_rows(grad_rows, routes, weights, n_experts, capacity):
    feature_width = grad_rows.shape[1]
    scaled = (grad_rows.astype(jnp.float32)[:, None, :] * weights.astype(jnp.float32)[:, :, None]).reshape(-1, feature_width)
    positions = slot_index(routes, n_experts, capacity)
    blank_rows = jnp.zeros((n_experts * capacity, feature_width), jnp.float32)
    return blank_rows.at[positions].set(scaled).astype(jnp.bfloat16)


def place_rows(inputs, routes, n_experts, capacity):
    feature_width = inputs.shape[1]
    chosen = routes.shape[1]
    copies = jnp.broadcast_to(inputs[:, None, :], (inputs.shape[0], chosen, feature_width)).reshape(-1, feature_width)
    positions = slot_index(routes, n_experts, capacity)
    blank_rows = jnp.zeros((n_experts * capacity, feature_width), inputs.dtype)
    return blank_rows.at[positions].set(copies)


def activations(gate_pre, up_pre, grad_hidden):
    sigmoid_gate = jax.nn.sigmoid(gate_pre)
    activated = gate_pre * sigmoid_gate
    hidden = (activated * up_pre).astype(jnp.bfloat16)
    slope_term = sigmoid_gate * (1.0 + gate_pre * (1.0 - sigmoid_gate))
    d_gate = (grad_hidden * up_pre * slope_term).astype(jnp.bfloat16)
    d_up = (grad_hidden * activated).astype(jnp.bfloat16)
    return hidden, d_gate, d_up


def expert_backward(received, saved, gate_mat, up_mat, down_mat):
    gate_pre = jnp.dot(saved, gate_mat, preferred_element_type=jnp.float32)
    up_pre = jnp.dot(saved, up_mat, preferred_element_type=jnp.float32)
    grad_hidden = jnp.dot(received, down_mat, preferred_element_type=jnp.float32)
    hidden, d_gate, d_up = activations(gate_pre, up_pre, grad_hidden)
    block_width = FFW // SHARES
    back_parts = []
    for share_id in range(SHARES):
        start_col = share_id * block_width
        stop_col = start_col + block_width
        part_sum = (jnp.dot(d_gate[:, start_col:stop_col], gate_mat[:, start_col:stop_col].T, preferred_element_type=jnp.float32)
                    + jnp.dot(d_up[:, start_col:stop_col], up_mat[:, start_col:stop_col].T, preferred_element_type=jnp.float32))
        back_parts.append(part_sum.astype(jnp.bfloat16))
    back_rows = jnp.stack(back_parts, axis=0)
    grad_g = jnp.dot(saved.T, d_gate, preferred_element_type=jnp.float32).astype(jnp.bfloat16)
    grad_u = jnp.dot(saved.T, d_up, preferred_element_type=jnp.float32).astype(jnp.bfloat16)
    grad_d = jnp.dot(received.T, hidden, preferred_element_type=jnp.float32).astype(jnp.bfloat16)
    return back_rows, grad_g, grad_u, grad_d


def reference(token_grads, routing, gate_weights, layer_inputs, w_gate, w_up, w_down):
    n_experts = EXPERTS
    capacity = CAP
    upstream_list = []
    gate_list = []
    up_list = []
    down_list = []
    for section_id in range(N_SECTION):
        grad_rows = token_grads[section_id].reshape(N_EXPERT, TOK_DEV, D)
        inputs = layer_inputs[section_id].reshape(N_EXPERT, TOK_DEV, D)
        routes = routing[section_id].reshape(N_EXPERT, TOK_DEV, TOP)
        weights = gate_weights[section_id].reshape(N_EXPERT, TOK_DEV, TOP)

        def send_one(items):
            return (dispatch_rows(items[0], items[1], items[2], n_experts, capacity),
                    place_rows(items[3], items[1], n_experts, capacity))

        outgoing, placed = lax.map(send_one, (grad_rows, routes, weights, inputs))
        arrived = jnp.transpose(outgoing.reshape(N_EXPERT, n_experts, capacity, D), (1, 0, 2, 3)).reshape(n_experts, N_EXPERT * capacity, D)
        saved_all = jnp.transpose(placed.reshape(N_EXPERT, n_experts, capacity, D), (1, 0, 2, 3)).reshape(n_experts, N_EXPERT * capacity, D)

        def per_expert(matrix):
            return jnp.transpose(matrix.reshape(D, n_experts, FFW), (1, 0, 2))

        def expert_one(items):
            return expert_backward(items[0], items[1], items[2], items[3], items[4])

        back_rows, grad_g, grad_u, grad_d = lax.map(
            expert_one, (arrived, saved_all, per_expert(w_gate[section_id]), per_expert(w_up[section_id]), per_expert(w_down[section_id])))
        merged = jnp.sum(back_rows.astype(jnp.float32), axis=1)
        returned = jnp.transpose(merged.reshape(n_experts, N_EXPERT, capacity, D), (1, 0, 2, 3)).reshape(N_EXPERT, n_experts * capacity, D)

        def combine_one(items):
            table, group_routes = items
            positions = slot_index(group_routes, n_experts, capacity)
            picked = table[positions].reshape(TOK_DEV, TOP, D)
            return jnp.sum(picked, axis=1).astype(jnp.bfloat16)

        input_grad = lax.map(combine_one, (returned, routes)).reshape(TOKENS, D)

        def joined(grad_blocks):
            return jnp.transpose(grad_blocks, (1, 0, 2)).reshape(D, n_experts * FFW)

        upstream_list.append(input_grad)
        gate_list.append(joined(grad_g))
        up_list.append(joined(grad_u))
        down_list.append(joined(grad_d))
    shifted = upstream_list[1:] + [jnp.zeros((TOKENS, D), jnp.bfloat16)]
    return (jnp.stack(shifted, axis=0), jnp.stack(gate_list, axis=0),
            jnp.stack(up_list, axis=0), jnp.stack(down_list, axis=0))
```

```python
import functools

import jax
import jax.numpy as jnp
from jax import lax
from jax.experimental import pallas as pl
from jax.experimental.pallas import tpu as pltpu
from jax.sharding import PartitionSpec as P

SHARES = 4
F32 = jnp.float32
BF16 = jnp.bfloat16
VMEM_BYTES = 16 * 1024 * 1024


def round_up(value, multiple):
    return -(-value // multiple) * multiple


def call(body, out_shape, flops, n_bytes, scratch=()):
    return functools.partial(
        pl.pallas_call,
        out_shape=out_shape,
        scratch_shapes=list(scratch),
        compiler_params=pltpu.CompilerParams(vmem_limit_bytes=VMEM_BYTES),
        cost_estimate=pl.CostEstimate(flops=flops, bytes_accessed=n_bytes, transcendentals=0),
    )(body)


def dot(left, right, left_dim=1, right_dim=0):
    return lax.dot_general(
        left, right, (((left_dim,), (right_dim,)), ((), ())), preferred_element_type=F32
    )


def slots(routes, n_experts):
    chosen, n_tokens = routes.shape
    shift = lax.axis_index("expert") // SHARES
    relative = routes - shift
    relative = jnp.where(relative < 0, relative + n_experts, relative)
    experts = lax.broadcasted_iota(jnp.int32, (round_up(n_experts, 8), n_tokens), 0)
    named = [relative[k : k + 1] == experts for k in range(chosen)]
    count = sum(one.astype(F32) for one in named)
    earlier = (
        lax.broadcasted_iota(jnp.int32, (n_tokens, n_tokens), 0)
        < lax.broadcasted_iota(jnp.int32, (n_tokens, n_tokens), 1)
    ).astype(BF16)
    before = dot(count.astype(BF16), earlier)
    slot_rows = []
    for k in range(chosen):
        rank = jnp.sum(jnp.where(named[k], before, 0.0), axis=0, keepdims=True).astype(jnp.int32)
        for other in range(k):
            rank = rank + (relative[other : other + 1] == relative[k : k + 1]).astype(jnp.int32)
        slot_rows.append(rank)
    return relative, slot_rows


def dispatch_block(routes, weights, grad_rows, inputs, which, n_experts, capacity, split):
    chosen, n_tokens = routes.shape
    columns = inputs.shape[1]
    rows = round_up(2 * capacity, 8)

    def body(routes_ref, weights_ref, grads_ref, inputs_ref, lo_ref, hi_ref):
        relative, slot_rows = slots(routes_ref[...], n_experts)
        row = lax.broadcasted_iota(jnp.int32, (rows, n_tokens), 0)
        pick_input = jnp.zeros((rows, n_tokens), F32)
        pick_grad = jnp.zeros((rows, n_tokens), F32)
        scale = jnp.zeros((rows, n_tokens), F32)
        for k in range(chosen):
            target = jnp.where(relative[k : k + 1] == which, slot_rows[k], -2 * rows)
            pick_input = pick_input + (row == target).astype(F32)
            hit = (row == target + capacity).astype(F32)
            pick_grad = pick_grad + hit
            scale = scale + hit * weights_ref[k : k + 1, :]
        scale = jnp.sum(scale, axis=1, keepdims=True)
        pick_input = pick_input.astype(BF16)
        pick_grad = pick_grad.astype(BF16)
        for out_ref, begin, end in ((lo_ref, 0, split), (hi_ref, split, columns)):
            block = dot(pick_input, inputs_ref[:, begin:end])
            block = block + dot(pick_grad, grads_ref[:, begin:end]) * scale
            out_ref[...] = block.astype(BF16)

    return call(
        body,
        (
            jax.ShapeDtypeStruct((rows, split), BF16),
            jax.ShapeDtypeStruct((rows, columns - split), BF16),
        ),
        2 * 2 * rows * n_tokens * columns,
        2 * n_tokens * columns * 2 + rows * columns * 2,
    )(routes, weights, grad_rows, inputs)


def partial_products(blocks, gate_cols, up_cols, down_cols, capacity, split):
    rows = round_up(2 * capacity, 8)
    kept = round_up(capacity, 8)
    n_blocks = len(blocks)
    columns, width = gate_cols.shape

    def body(*refs):
        block_refs = refs[: 2 * n_blocks]
        gate_ref, up_ref, down_ref, out_ref, packed_ref = refs[2 * n_blocks :]
        for i in range(n_blocks):
            packed_ref[i * rows : (i + 1) * rows, :split] = block_refs[2 * i][...]
            packed_ref[i * rows : (i + 1) * rows, split:] = block_refs[2 * i + 1][...]
        packed = packed_ref[...]
        gate = dot(packed, gate_ref[...])
        up = dot(packed, up_ref[...])
        down = dot(packed, down_ref[...])
        for i in range(n_blocks):
            at = i * rows
            out_ref[i, :, :width] = gate[at : at + kept]
            out_ref[i, :, width : 2 * width] = up[at : at + kept]
            out_ref[i, :capacity, 2 * width :] = down[at + capacity : at + 2 * capacity]
            if kept > capacity:
                out_ref[i, capacity:, 2 * width :] = jnp.zeros((kept - capacity, width), F32)

    return call(
        body,
        (
            jax.ShapeDtypeStruct((n_blocks, kept, 3 * width), F32),
            jax.ShapeDtypeStruct((n_blocks * rows, columns), BF16),
        ),
        2 * 3 * n_blocks * rows * columns * width,
        3 * columns * width * 2 + n_blocks * rows * columns * 4,
    )(*[half for block in blocks for half in block], gate_cols, up_cols, down_cols)


def hidden_backward(partials, gate_cols, up_cols, capacity):
    n_blocks, kept, width3 = partials[0].shape
    columns, width = gate_cols.shape
    rows = round_up(2 * capacity, 8)
    n_parts = len(partials)

    def body(*refs):
        part_refs = refs[:n_parts]
        gate_ref, up_ref = refs[n_parts : n_parts + 2]
        back_refs = refs[n_parts + 2 : n_parts + 2 + n_blocks]
        slope_ref = refs[n_parts + 2 + n_blocks]
        valid = lax.broadcasted_iota(jnp.int32, (kept, width), 0) < capacity
        d_gates, d_ups = [], []
        slope_ref[...] = jnp.zeros(slope_ref.shape, BF16)
        for i in range(n_blocks):
            total = part_refs[0][i]
            for ref in part_refs[1:]:
                total = total + ref[i]
            gate = jnp.where(valid, total[:, :width], 0.0)
            up = jnp.where(valid, total[:, width : 2 * width], 0.0)
            grad_hidden = total[:, 2 * width :]
            sigmoid_gate = jax.nn.sigmoid(gate)
            activated = gate * sigmoid_gate
            hidden = (activated * up).astype(BF16)
            slope_term = sigmoid_gate * (1.0 + gate * (1.0 - sigmoid_gate))
            d_gate = (grad_hidden * up * slope_term).astype(BF16)
            d_up = (grad_hidden * activated).astype(BF16)
            at = i * rows
            slope_ref[at : at + capacity, :width] = d_gate[:capacity]
            slope_ref[at : at + capacity, width : 2 * width] = d_up[:capacity]
            slope_ref[at + capacity : at + 2 * capacity, 2 * width :] = hidden[:capacity]
            d_gates.append(d_gate)
            d_ups.append(d_up)
        back = dot(jnp.concatenate(d_gates, axis=0), gate_ref[...], 1, 1)
        back = back + dot(jnp.concatenate(d_ups, axis=0), up_ref[...], 1, 1)
        for i in range(n_blocks):
            back_refs[i][...] = back[i * kept : (i + 1) * kept].astype(BF16)

    outs = call(
        body,
        tuple(jax.ShapeDtypeStruct((kept, columns), BF16) for _ in range(n_blocks))
        + (jax.ShapeDtypeStruct((n_blocks * rows, width3), BF16),),
        2 * 2 * n_blocks * kept * columns * width,
        2 * columns * width * 2 + n_blocks * kept * columns * 2,
    )(*partials, gate_cols, up_cols)
    return outs[:n_blocks], outs[n_blocks]


def weight_grads(packed, slopes, width):
    columns = packed[0].shape[1]
    n_parts = len(packed)
    n_rows = sum(one.shape[0] for one in packed)

    def body(*refs):
        packed_refs = refs[:n_parts]
        slope_refs = refs[n_parts : 2 * n_parts]
        out_refs = refs[2 * n_parts :]
        total = dot(packed_refs[0][...], slope_refs[0][...], 0, 0)
        for left, right in zip(packed_refs[1:], slope_refs[1:]):
            total = total + dot(left[...], right[...], 0, 0)
        for i in range(3):
            out_refs[i][...] = total[:, i * width : (i + 1) * width].astype(BF16)

    return call(
        body,
        tuple(jax.ShapeDtypeStruct((columns, width), BF16) for _ in range(3)),
        2 * 3 * n_rows * columns * width,
        3 * columns * width * 2 + n_rows * columns * 2,
    )(*packed, *slopes)


def combine(routes, merged, n_experts, capacity):
    chosen, n_tokens = routes.shape
    kept, columns = merged[0].shape

    def body(routes_ref, *refs):
        merged_refs, out_ref = refs[:-1], refs[-1]
        relative, slot_rows = slots(routes_ref[...], n_experts)
        row = lax.broadcasted_iota(jnp.int32, (kept, n_tokens), 0)
        total = None
        for which, ref in enumerate(merged_refs):
            pick = jnp.zeros((kept, n_tokens), F32)
            for k in range(chosen):
                target = jnp.where(relative[k : k + 1] == which, slot_rows[k], -1)
                pick = pick + (row == target).astype(F32)
            term = dot(pick.astype(BF16), ref[...], 0, 0)
            total = term if total is None else total + term
        out_ref[...] = total.astype(BF16)

    return call(
        body,
        jax.ShapeDtypeStruct((n_tokens, columns), BF16),
        2 * n_tokens * columns * kept * len(merged),
        kept * columns * 2 * len(merged) + n_tokens * columns * 2,
    )(routes, *merged)


def per_device(token_grads, routing, gate_weights, layer_inputs, w_gate, w_up, w_down):
    n_groups = lax.axis_size("expert")
    n_sections = lax.axis_size("section")
    n_replicas = lax.axis_size("replica")
    n_experts = n_groups // SHARES
    grad_rows, inputs = token_grads[0], layer_inputs[0]
    routes, weights = routing[0].T, gate_weights[0].T
    gate_cols, up_cols, down_cols = w_gate[0], w_up[0], w_down[0]
    chosen, n_tokens = routes.shape
    columns = inputs.shape[1]
    width = gate_cols.shape[1]
    capacity = min(n_tokens, 17 * n_tokens * chosen // (16 * n_experts))
    split = round_up(columns // 2, 128)

    def partner(value, step):
        return lax.ppermute(value, "expert", [(j, j ^ step) for j in range(n_groups)])

    def partner_back(value, step):
        pairs = [
            (s * n_groups + j, s * n_groups + (j ^ step))
            for s in range(1, n_sections)
            for j in range(n_groups)
        ]
        return lax.ppermute(value, ("section", "expert"), pairs)

    def dispatch(which):
        return dispatch_block(
            routes, weights, grad_rows, inputs, which, n_experts, capacity, split
        )

    def crossing(value, which):
        move = SHARES * which
        return lax.ppermute(
            value, "expert", [(j, (j + move) % n_groups) for j in range(n_groups)]
        )

    routes_next = lax.ppermute(
        routes, "section", [(s, s - 1) for s in range(1, n_sections)]
    )

    heads = [None] * n_experts
    for which in list(range(1, n_experts)) + [0]:
        lo, hi = dispatch(which)
        heads[which] = (crossing(lo, which), crossing(hi, which)) if which else (lo, hi)

    packed, slopes, merged = [], [], []
    for which in range(n_experts):
        lo, hi = heads[which]
        lo_y, hi_y = partner(lo, 1), partner(hi, 1)
        lo_z, hi_z = partner(lo, 2), partner(hi, 2)
        if which == 0:
            lo_d, hi_d = partner(lo_z, 1), partner(hi_z, 1)
        else:
            lo_d, hi_d = partner(lo_z, 1), partner(hi_y, 2)
        blocks = ((lo, hi), (lo_y, hi_y), (lo_z, hi_z), (lo_d, hi_d))
        part, rows_packed = partial_products(
            blocks, gate_cols, up_cols, down_cols, capacity, split
        )
        parts = [part]
        for turn in range(1, n_replicas):
            parts.append(
                lax.ppermute(
                    part, "replica", [(r, (r + turn) % n_replicas) for r in range(n_replicas)]
                )
            )
        backs, slope = hidden_backward(parts, gate_cols, up_cols, capacity)
        packed.append(rows_packed)
        slopes.append(slope)
        total = backs[0].astype(F32)
        for step in range(1, SHARES):
            total = total + partner_back(backs[step], step).astype(F32)
        move = SHARES * which
        home = [
            (s * n_groups + j, (s - 1) * n_groups + (j - move) % n_groups)
            for s in range(1, n_sections)
            for j in range(n_groups)
        ]
        merged.append(lax.ppermute(total.astype(BF16), ("section", "expert"), home))

    upstream = combine(routes_next, merged, n_experts, capacity)
    grad_gate, grad_up, grad_down = weight_grads(packed, slopes, width)
    return (upstream[None], grad_gate[None], grad_up[None], grad_down[None])


def solution(mesh):
    placed = (
        P("section", "expert", "replica"),
        P("section", "expert", None),
        P("section", "expert", None),
        P("section", "expert", "replica"),
        P("section", "replica", "expert"),
        P("section", "replica", "expert"),
        P("section", "replica", "expert"),
    )
    return jax.shard_map(
        per_device,
        mesh=mesh,
        in_specs=placed,
        out_specs=(
            P("section", "expert", "replica"),
            P("section", "replica", "expert"),
            P("section", "replica", "expert"),
            P("section", "replica", "expert"),
        ),
        check_vma=False,
    )
```

```python
import functools

import jax
import jax.numpy as jnp
from jax import lax
from jax.experimental import pallas as pl
from jax.experimental.pallas import tpu as pltpu
from jax.sharding import PartitionSpec as P

SHARES = 4
F32 = jnp.float32
BF16 = jnp.bfloat16
VMEM_BYTES = 16 * 1024 * 1024


def round_up(value, multiple):
    return -(-value // multiple) * multiple


def call(body, out_shape, flops, n_bytes, scratch=(), in_specs=None):
    placed = {} if in_specs is None else {"in_specs": in_specs}
    return functools.partial(
        pl.pallas_call,
        out_shape=out_shape,
        scratch_shapes=list(scratch),
        **placed,
        compiler_params=pltpu.CompilerParams(vmem_limit_bytes=VMEM_BYTES),
        cost_estimate=pl.CostEstimate(flops=flops, bytes_accessed=n_bytes, transcendentals=0),
    )(body)


def dot(left, right, left_dim=1, right_dim=0):
    return lax.dot_general(
        left, right, (((left_dim,), (right_dim,)), ((), ())), preferred_element_type=F32
    )


def slots(routes, n_experts):
    chosen, n_tokens = routes.shape
    shift = lax.axis_index("expert") // SHARES
    relative = routes - shift
    relative = jnp.where(relative < 0, relative + n_experts, relative)
    experts = lax.broadcasted_iota(jnp.int32, (round_up(n_experts, 8), n_tokens), 0)
    named = [relative[k : k + 1] == experts for k in range(chosen)]
    count = sum(one.astype(F32) for one in named)
    earlier = (
        lax.broadcasted_iota(jnp.int32, (n_tokens, n_tokens), 0)
        < lax.broadcasted_iota(jnp.int32, (n_tokens, n_tokens), 1)
    ).astype(BF16)
    before = dot(count.astype(BF16), earlier)
    slot_rows = []
    for k in range(chosen):
        rank = jnp.sum(jnp.where(named[k], before, 0.0), axis=0, keepdims=True).astype(jnp.int32)
        for other in range(k):
            rank = rank + (relative[other : other + 1] == relative[k : k + 1]).astype(jnp.int32)
        slot_rows.append(rank)
    return relative, slot_rows


def dispatch_blocks(routes, weights, grad_rows, inputs, n_experts, capacity, split):
    chosen, n_tokens = routes.shape
    columns = inputs.shape[1]
    rows = round_up(2 * capacity, 8)
    order = list(range(1, n_experts)) + [0]

    def body(routes_ref, weights_ref, grads_hbm, inputs_hbm, *refs):
        out_refs = refs[: 2 * n_experts]
        grads_ref, inputs_ref, sems = refs[2 * n_experts :]
        copies = [
            pltpu.make_async_copy(inputs_hbm, inputs_ref, sems.at[0]),
            pltpu.make_async_copy(grads_hbm, grads_ref, sems.at[1]),
        ]
        for copy in copies:
            copy.start()
        relative, slot_rows = slots(routes_ref[...], n_experts)
        row = lax.broadcasted_iota(jnp.int32, (rows, n_tokens), 0)
        for copy in copies:
            copy.wait()
        for which in order:
            pick_input = jnp.zeros((rows, n_tokens), F32)
            pick_grad = jnp.zeros((rows, n_tokens), F32)
            scale = jnp.zeros((rows, n_tokens), F32)
            for k in range(chosen):
                target = jnp.where(relative[k : k + 1] == which, slot_rows[k], -2 * rows)
                pick_input = pick_input + (row == target).astype(F32)
                hit = (row == target + capacity).astype(F32)
                pick_grad = pick_grad + hit
                scale = scale + hit * weights_ref[k : k + 1, :]
            scale = jnp.sum(scale, axis=1, keepdims=True)
            pick_input = pick_input.astype(BF16)
            pick_grad = pick_grad.astype(BF16)
            for part, (begin, end) in enumerate(((0, split), (split, columns))):
                block = dot(pick_input, inputs_ref[:, begin:end])
                block = block + dot(pick_grad, grads_ref[:, begin:end]) * scale
                out_refs[2 * which + part][...] = block.astype(BF16)

    shapes = (
        jax.ShapeDtypeStruct((rows, split), BF16),
        jax.ShapeDtypeStruct((rows, columns - split), BF16),
    )
    in_vmem, in_hbm = pl.BlockSpec(memory_space=pltpu.VMEM), pl.BlockSpec(memory_space=pltpu.HBM)
    outs = call(
        body,
        shapes * n_experts,
        2 * 2 * n_experts * rows * n_tokens * columns,
        2 * n_tokens * columns * 2 + n_experts * rows * columns * 2,
        [
            pltpu.VMEM((n_tokens, columns), BF16),
            pltpu.VMEM((n_tokens, columns), BF16),
            pltpu.SemaphoreType.DMA((2,)),
        ],
        [in_vmem, in_vmem, in_hbm, in_hbm],
    )(routes, weights, grad_rows, inputs)
    return [(outs[2 * which], outs[2 * which + 1]) for which in range(n_experts)]


def stage_weights(gate_cols, up_cols, down_cols):
    columns, width = gate_cols.shape

    def body(gate_hbm, up_hbm, down_hbm, out_ref, sems):
        copies = [
            pltpu.make_async_copy(ref, out_ref.at[:, i * width : (i + 1) * width], sems.at[i])
            for i, ref in enumerate((gate_hbm, up_hbm, down_hbm))
        ]
        for copy in copies:
            copy.start()
        for copy in copies:
            copy.wait()

    return call(
        body,
        jax.ShapeDtypeStruct((columns, 3 * width), BF16),
        2 * columns * width * 256,
        6 * columns * width * 2,
        [pltpu.SemaphoreType.DMA((3,))],
        [pl.BlockSpec(memory_space=pltpu.HBM)] * 3,
    )(gate_cols, up_cols, down_cols)


def partial_products(blocks, staged, capacity, split):
    rows = round_up(2 * capacity, 8)
    kept = round_up(capacity, 8)
    n_blocks = len(blocks)
    columns, width = staged.shape[0], staged.shape[1] // 3

    def body(*refs):
        block_refs = refs[: 2 * n_blocks]
        staged_ref, out_ref, packed_ref = refs[2 * n_blocks :]
        for i in range(n_blocks):
            packed_ref[i * rows : (i + 1) * rows, :split] = block_refs[2 * i][...]
            packed_ref[i * rows : (i + 1) * rows, split:] = block_refs[2 * i + 1][...]
        packed = packed_ref[...]
        gate_up = dot(packed, staged_ref[:, : 2 * width])
        down = dot(packed, staged_ref[:, 2 * width :])
        for i in range(n_blocks):
            at = i * rows
            out_ref[i, :, : 2 * width] = gate_up[at : at + kept]
            out_ref[i, :capacity, 2 * width :] = down[at + capacity : at + 2 * capacity]
            if kept > capacity:
                out_ref[i, capacity:, 2 * width :] = jnp.zeros((kept - capacity, width), F32)

    return call(
        body,
        (
            jax.ShapeDtypeStruct((n_blocks, kept, 3 * width), F32),
            jax.ShapeDtypeStruct((n_blocks * rows, columns), BF16),
        ),
        2 * 3 * n_blocks * rows * columns * width,
        3 * columns * width * 2 + n_blocks * rows * columns * 4,
    )(*[half for block in blocks for half in block], staged)


def hidden_backward(partials, staged, capacity, split):
    n_blocks, kept, width3 = partials[0].shape
    columns, width = staged.shape[0], staged.shape[1] // 3
    rows = round_up(2 * capacity, 8)
    n_parts = len(partials)

    def body(*refs):
        part_refs = refs[:n_parts]
        staged_ref = refs[n_parts]
        back_refs = refs[n_parts + 1 : n_parts + 1 + n_blocks]
        slope_ref = refs[n_parts + 1 + n_blocks]
        valid = lax.broadcasted_iota(jnp.int32, (kept, width), 0) < capacity
        d_gates, d_ups = [], []
        slope_ref[...] = jnp.zeros(slope_ref.shape, BF16)
        for i in range(n_blocks):
            total = part_refs[0][i]
            for ref in part_refs[1:]:
                total = total + ref[i]
            gate = jnp.where(valid, total[:, :width], 0.0)
            up = jnp.where(valid, total[:, width : 2 * width], 0.0)
            grad_hidden = total[:, 2 * width :]
            sigmoid_gate = jax.nn.sigmoid(gate)
            activated = gate * sigmoid_gate
            hidden = (activated * up).astype(BF16)
            slope_term = sigmoid_gate * (1.0 + gate * (1.0 - sigmoid_gate))
            d_gate = (grad_hidden * up * slope_term).astype(BF16)
            d_up = (grad_hidden * activated).astype(BF16)
            at = i * rows
            slope_ref[at : at + capacity, :width] = d_gate[:capacity]
            slope_ref[at : at + capacity, width : 2 * width] = d_up[:capacity]
            slope_ref[at + capacity : at + 2 * capacity, 2 * width :] = hidden[:capacity]
            d_gates.append(d_gate)
            d_ups.append(d_up)
        slope = jnp.concatenate(
            [jnp.concatenate(d_gates, axis=0), jnp.concatenate(d_ups, axis=0)], axis=1
        )
        back = dot(slope, staged_ref[:, : 2 * width], 1, 1)
        for i in range(n_blocks):
            part = back[i * kept : i * kept + capacity].astype(BF16)
            back_refs[i][:capacity, :] = part[:, :split]
            back_refs[i][capacity : 2 * capacity, : columns - split] = part[:, split:]
            if columns < 2 * split:
                back_refs[i][capacity : 2 * capacity, columns - split :] = jnp.zeros(
                    (capacity, 2 * split - columns), BF16
                )
            if rows > 2 * capacity:
                back_refs[i][2 * capacity :, :] = jnp.zeros((rows - 2 * capacity, split), BF16)

    outs = call(
        body,
        tuple(jax.ShapeDtypeStruct((rows, split), BF16) for _ in range(n_blocks))
        + (jax.ShapeDtypeStruct((n_blocks * rows, width3), BF16),),
        2 * 2 * n_blocks * kept * columns * width,
        2 * columns * width * 2 + n_blocks * kept * columns * 2,
    )(*partials, staged)
    return outs[:n_blocks], outs[n_blocks]


def weight_grads(packed, slopes, width):
    columns = packed[0].shape[1]
    n_parts = len(packed)
    n_rows = sum(one.shape[0] for one in packed)

    def body(*refs):
        packed_refs = refs[:n_parts]
        slope_refs = refs[n_parts : 2 * n_parts]
        out_refs = refs[2 * n_parts :]
        total = dot(packed_refs[0][...], slope_refs[0][...], 0, 0)
        for left, right in zip(packed_refs[1:], slope_refs[1:]):
            total = total + dot(left[...], right[...], 0, 0)
        for i in range(3):
            out_refs[i][...] = total[:, i * width : (i + 1) * width].astype(BF16)

    return call(
        body,
        tuple(jax.ShapeDtypeStruct((columns, width), BF16) for _ in range(3)),
        2 * 3 * n_rows * columns * width,
        3 * columns * width * 2 + n_rows * columns * 2,
    )(*packed, *slopes)


def combine(routes, merged, n_experts, capacity, columns):
    chosen, n_tokens = routes.shape
    rows, split = merged[0].shape

    def body(routes_ref, *refs):
        merged_refs, out_ref = refs[:-1], refs[-1]
        relative, slot_rows = slots(routes_ref[...], n_experts)
        row = lax.broadcasted_iota(jnp.int32, (rows, n_tokens), 0)
        last = lax.axis_index("section") == lax.axis_size("section") - 1
        for offset, begin, end in ((0, 0, split), (capacity, split, columns)):
            total = jnp.zeros((n_tokens, end - begin), F32)
            for which, ref in enumerate(merged_refs):
                pick = jnp.zeros((rows, n_tokens), F32)
                for k in range(chosen):
                    target = jnp.where(relative[k : k + 1] == which, slot_rows[k], -2 * rows)
                    pick = pick + (row == target + offset).astype(F32)
                total = total + dot(pick.astype(BF16), ref[:, : end - begin], 0, 0)
            out_ref[:, begin:end] = jnp.where(last, 0.0, total).astype(BF16)

    return call(
        body,
        jax.ShapeDtypeStruct((n_tokens, columns), BF16),
        2 * 2 * n_tokens * columns * rows * len(merged),
        rows * columns * 2 * len(merged) + n_tokens * columns * 2,
    )(routes, *merged)


def per_device(token_grads, routing, gate_weights, layer_inputs, w_gate, w_up, w_down):
    n_groups = lax.axis_size("expert")
    n_sections = lax.axis_size("section")
    n_replicas = lax.axis_size("replica")
    n_experts = n_groups // SHARES
    grad_rows, inputs = token_grads[0], layer_inputs[0]
    routes, weights = routing[0].T, gate_weights[0].T
    gate_cols, up_cols, down_cols = w_gate[0], w_up[0], w_down[0]
    chosen, n_tokens = routes.shape
    columns = inputs.shape[1]
    width = gate_cols.shape[1]
    capacity = min(n_tokens, 17 * n_tokens * chosen // (16 * n_experts))
    split = round_up(columns // 2, 128)

    def partner(value, step):
        return lax.ppermute(value, "expert", [(j, j ^ step) for j in range(n_groups)])

    def crossing(value, which):
        move = SHARES * which
        return lax.ppermute(
            value, "expert", [(j, (j + move) % n_groups) for j in range(n_groups)]
        )

    def homeward(value, which):
        move = SHARES * which
        pairs = [
            (s * n_groups + j, (s - 1) % n_sections * n_groups + (j - move) % n_groups)
            for s in range(n_sections)
            for j in range(n_groups)
        ]
        return lax.ppermute(value, ("section", "expert"), pairs)

    routes_next = lax.ppermute(
        routes, "section", [(s, (s - 1) % n_sections) for s in range(n_sections)]
    )
    own = dispatch_blocks(routes, weights, grad_rows, inputs, n_experts, capacity, split)
    staged = stage_weights(gate_cols, up_cols, down_cols)
    heads = [own[0]] + [
        tuple(crossing(part, which) for part in own[which]) for which in range(1, n_experts)
    ]

    packed, slopes, merged = [], [], []
    for which in range(n_experts):
        lo, hi = heads[which]
        lo_y, hi_y = partner(lo, 1), partner(hi, 1)
        lo_z, hi_z = partner(lo, 2), partner(hi, 2)
        if which == 0:
            lo_d, hi_d = partner(lo_z, 1), partner(hi_z, 1)
        else:
            lo_d, hi_d = partner(lo_z, 1), partner(hi_y, 2)
        blocks = ((lo, hi), (lo_y, hi_y), (lo_z, hi_z), (lo_d, hi_d))
        part, rows_packed = partial_products(blocks, staged, capacity, split)
        parts = [part]
        for turn in range(1, n_replicas):
            parts.append(
                lax.ppermute(
                    part, "replica", [(r, (r + turn) % n_replicas) for r in range(n_replicas)]
                )
            )
        backs, slope = hidden_backward(parts, staged, capacity, split)
        packed.append(rows_packed)
        slopes.append(slope)
        total = backs[0].astype(F32)
        for step in range(1, SHARES):
            total = total + partner(backs[step], step).astype(F32)
        merged.append(homeward(total.astype(BF16), which))

    upstream = combine(routes_next, merged, n_experts, capacity, columns)
    grad_gate, grad_up, grad_down = weight_grads(packed, slopes, width)
    return (upstream[None], grad_gate[None], grad_up[None], grad_down[None])


def solution(mesh):
    placed = (
        P("section", "expert", "replica"),
        P("section", "expert", None),
        P("section", "expert", None),
        P("section", "expert", "replica"),
        P("section", "replica", "expert"),
        P("section", "replica", "expert"),
        P("section", "replica", "expert"),
    )
    return jax.shard_map(
        per_device,
        mesh=mesh,
        in_specs=placed,
        out_specs=(
            P("section", "expert", "replica"),
            P("section", "replica", "expert"),
            P("section", "replica", "expert"),
            P("section", "replica", "expert"),
        ),
        check_vma=False,
    )
```

```python
import functools

import jax
import jax.numpy as jnp
from jax import lax
from jax.experimental import pallas as pl
from jax.experimental.pallas import tpu as pltpu
from jax.sharding import PartitionSpec as P


SHARES = 4
F32 = jnp.float32
BF16 = jnp.bfloat16
VMEM_BYTES = 16 * 1024 * 1024


def round_up(value, multiple):
    return -(-value // multiple) * multiple


def call(body, out_shape, flops, n_bytes, scratch=(), in_specs=None):
    placed = {} if in_specs is None else {"in_specs": in_specs}
    return functools.partial(
        pl.pallas_call,
        out_shape=out_shape,
        scratch_shapes=list(scratch),
        **placed,
        compiler_params=pltpu.CompilerParams(vmem_limit_bytes=VMEM_BYTES),
        cost_estimate=pl.CostEstimate(flops=flops, bytes_accessed=n_bytes, transcendentals=0),
    )(body)


def in_hbm(value):
    return pltpu.with_memory_space_constraint(value, pltpu.HBM)


def dot(left, right, left_dim=1, right_dim=0):
    return lax.dot_general(
        left, right, (((left_dim,), (right_dim,)), ((), ())), preferred_element_type=F32
    )


def slots(routes, n_experts):
    chosen, n_tokens = routes.shape
    shift = lax.axis_index("expert") // SHARES
    relative = routes - shift
    relative = jnp.where(relative < 0, relative + n_experts, relative)
    experts = lax.broadcasted_iota(jnp.int32, (round_up(n_experts, 8), n_tokens), 0)
    named = [relative[k : k + 1] == experts for k in range(chosen)]
    count = sum(one.astype(F32) for one in named)
    earlier = (
        lax.broadcasted_iota(jnp.int32, (n_tokens, n_tokens), 0)
        < lax.broadcasted_iota(jnp.int32, (n_tokens, n_tokens), 1)
    ).astype(BF16)
    before = dot(count.astype(BF16), earlier)
    slot_rows = []
    for k in range(chosen):
        rank = jnp.sum(jnp.where(named[k], before, 0.0), axis=0, keepdims=True).astype(jnp.int32)
        for other in range(k):
            rank = rank + (relative[other : other + 1] == relative[k : k + 1]).astype(jnp.int32)
        slot_rows.append(rank)
    return relative, slot_rows


def dispatch_blocks(routes, weights, grad_rows, inputs, cuts, capacity):
    n_experts = len(cuts)
    chosen, n_tokens = routes.shape
    columns = inputs.shape[1]
    rows = round_up(2 * capacity, 8)
    order = list(range(1, n_experts)) + [0]

    operands = (routes, weights, inputs, grad_rows)
    first = [sum(len(one) for one in cuts[:which]) for which in range(n_experts)]
    n_outs = first[-1] + len(cuts[-1])

    def body(*refs):
        out_refs = list(refs[len(operands) : len(operands) + n_outs])
        *held, sems = refs[len(operands) + n_outs :]
        routes_ref, weights_ref, inputs_ref, grads_ref = held
        copies = [
            pltpu.make_async_copy(source, target, sems.at[i])
            for i, (source, target) in enumerate(zip(refs, held))
        ]
        for copy in copies:
            copy.start()
        copies[0].wait()
        relative, slot_rows = slots(routes_ref[...], n_experts)
        row = lax.broadcasted_iota(jnp.int32, (rows, n_tokens), 0)
        for copy in copies[1:]:
            copy.wait()
        for which in order:
            pick_input = jnp.zeros((rows, n_tokens), F32)
            pick_grad = jnp.zeros((rows, n_tokens), F32)
            scale = jnp.zeros((rows, n_tokens), F32)
            for k in range(chosen):
                target = jnp.where(relative[k : k + 1] == which, slot_rows[k], -2 * rows)
                pick_input = pick_input + (row == target).astype(F32)
                hit = (row == target + capacity).astype(F32)
                pick_grad = pick_grad + hit
                scale = scale + hit * weights_ref[k : k + 1, :]
            scale = jnp.sum(scale, axis=1, keepdims=True)
            pick_input = pick_input.astype(BF16)
            pick_grad = pick_grad.astype(BF16)
            for part, (begin, end) in enumerate(cuts[which]):
                block = dot(pick_input, inputs_ref[:, begin:end])
                block = block + dot(pick_grad, grads_ref[:, begin:end]) * scale
                out_refs[first[which] + part][...] = block.astype(BF16)

    outs = call(
        body,
        tuple(
            jax.ShapeDtypeStruct((rows, end - begin), BF16) for one in cuts for begin, end in one
        ),
        2 * 2 * n_experts * rows * n_tokens * columns,
        2 * n_tokens * columns * 2 + n_experts * rows * columns * 2,
        [pltpu.VMEM(value.shape, value.dtype) for value in operands]
        + [pltpu.SemaphoreType.DMA((len(operands),))],
        [pl.BlockSpec(memory_space=pltpu.HBM)] * len(operands),
    )(*(in_hbm(value) for value in operands))
    return [
        list(outs[first[which] : first[which] + len(cuts[which])]) for which in range(n_experts)
    ]


def stage_weights(gate_cols, up_cols, down_cols):
    columns, width = gate_cols.shape

    def body(gate_hbm, up_hbm, down_hbm, out_ref, sems):
        copies = [
            pltpu.make_async_copy(ref, out_ref.at[:, i * width : (i + 1) * width], sems.at[i])
            for i, ref in enumerate((gate_hbm, up_hbm, down_hbm))
        ]
        for copy in copies:
            copy.start()
        for copy in copies:
            copy.wait()

    return call(
        body,
        jax.ShapeDtypeStruct((columns, 3 * width), BF16),
        2 * columns * width * 256,
        6 * columns * width * 2,
        [pltpu.SemaphoreType.DMA((3,))],
        [pl.BlockSpec(memory_space=pltpu.HBM)] * 3,
    )(*(in_hbm(value) for value in (gate_cols, up_cols, down_cols)))


def partial_products(blocks, staged, cuts, capacity):
    rows = round_up(2 * capacity, 8)
    kept = round_up(capacity, 8)
    n_blocks = len(blocks)
    columns, width = staged.shape[0], staged.shape[1] // 3

    def body(*refs):
        block_refs = refs[: n_blocks * len(cuts)]
        staged_ref, out_ref, packed_ref = refs[n_blocks * len(cuts) :]
        for i in range(n_blocks):
            for part, (begin, end) in enumerate(cuts):
                ref = block_refs[i * len(cuts) + part]
                packed_ref[i * rows : (i + 1) * rows, begin:end] = ref[...]
        packed = packed_ref[...]
        gate_up = dot(packed, staged_ref[:, : 2 * width])
        down = dot(packed, staged_ref[:, 2 * width :])
        for i in range(n_blocks):
            at = i * rows
            out_ref[i, :, : 2 * width] = gate_up[at : at + kept]
            out_ref[i, :capacity, 2 * width :] = down[at + capacity : at + 2 * capacity]
            if kept > capacity:
                out_ref[i, capacity:, 2 * width :] = jnp.zeros((kept - capacity, width), F32)

    return call(
        body,
        (
            jax.ShapeDtypeStruct((n_blocks, kept, 3 * width), F32),
            jax.ShapeDtypeStruct((n_blocks * rows, columns), BF16),
        ),
        2 * 3 * n_blocks * rows * columns * width,
        3 * columns * width * 2 + n_blocks * rows * columns * 4,
    )(*[part for block in blocks for part in block], staged)


def hidden_backward(partials, staged, capacity, split):
    n_blocks, kept, width3 = partials[0].shape
    columns, width = staged.shape[0], staged.shape[1] // 3
    rows = round_up(2 * capacity, 8)
    n_parts = len(partials)

    def body(*refs):
        part_refs = refs[:n_parts]
        staged_ref = refs[n_parts]
        back_refs = refs[n_parts + 1 : n_parts + 1 + n_blocks]
        slope_ref = refs[n_parts + 1 + n_blocks]
        valid = lax.broadcasted_iota(jnp.int32, (kept, width), 0) < capacity
        d_gates, d_ups = [], []
        slope_ref[...] = jnp.zeros(slope_ref.shape, BF16)
        for i in range(n_blocks):
            total = part_refs[0][i]
            for ref in part_refs[1:]:
                total = total + ref[i]
            gate = jnp.where(valid, total[:, :width], 0.0)
            up = jnp.where(valid, total[:, width : 2 * width], 0.0)
            grad_hidden = total[:, 2 * width :]
            sigmoid_gate = jax.nn.sigmoid(gate)
            activated = gate * sigmoid_gate
            hidden = (activated * up).astype(BF16)
            slope_term = sigmoid_gate * (1.0 + gate * (1.0 - sigmoid_gate))
            d_gate = (grad_hidden * up * slope_term).astype(BF16)
            d_up = (grad_hidden * activated).astype(BF16)
            at = i * rows
            slope_ref[at : at + capacity, :width] = d_gate[:capacity]
            slope_ref[at : at + capacity, width : 2 * width] = d_up[:capacity]
            slope_ref[at + capacity : at + 2 * capacity, 2 * width :] = hidden[:capacity]
            d_gates.append(d_gate)
            d_ups.append(d_up)
        slope = jnp.concatenate(
            [jnp.concatenate(d_gates, axis=0), jnp.concatenate(d_ups, axis=0)], axis=1
        )
        back = dot(slope, staged_ref[:, : 2 * width], 1, 1)
        for i in range(n_blocks):
            part = back[i * kept : i * kept + capacity].astype(BF16)
            back_refs[i][:capacity, :] = part[:, :split]
            back_refs[i][capacity : 2 * capacity, : columns - split] = part[:, split:]
            if columns < 2 * split:
                back_refs[i][capacity : 2 * capacity, columns - split :] = jnp.zeros(
                    (capacity, 2 * split - columns), BF16
                )
            if rows > 2 * capacity:
                back_refs[i][2 * capacity :, :] = jnp.zeros((rows - 2 * capacity, split), BF16)

    outs = call(
        body,
        tuple(jax.ShapeDtypeStruct((rows, split), BF16) for _ in range(n_blocks))
        + (jax.ShapeDtypeStruct((n_blocks * rows, width3), BF16),),
        2 * 2 * n_blocks * kept * columns * width,
        2 * columns * width * 2 + n_blocks * kept * columns * 2,
    )(*partials, staged)
    return outs[:n_blocks], outs[n_blocks]


def weight_grads(packed, slopes, width):
    columns = packed[0].shape[1]
    n_parts = len(packed)
    n_rows = sum(one.shape[0] for one in packed)

    def body(*refs):
        packed_refs = refs[:n_parts]
        slope_refs = refs[n_parts : 2 * n_parts]
        out_refs = refs[2 * n_parts :]
        total = dot(packed_refs[0][...], slope_refs[0][...], 0, 0)
        for left, right in zip(packed_refs[1:], slope_refs[1:]):
            total = total + dot(left[...], right[...], 0, 0)
        for i in range(3):
            out_refs[i][...] = total[:, i * width : (i + 1) * width].astype(BF16)

    return call(
        body,
        tuple(jax.ShapeDtypeStruct((columns, width), BF16) for _ in range(3)),
        2 * 3 * n_rows * columns * width,
        3 * columns * width * 2 + n_rows * columns * 2,
    )(*packed, *slopes)


def combine(routes, merged, n_experts, capacity, columns):
    chosen, n_tokens = routes.shape
    rows, split = merged[0].shape

    def body(routes_ref, *refs):
        merged_refs, out_ref = refs[:-1], refs[-1]
        relative, slot_rows = slots(routes_ref[...], n_experts)
        row = lax.broadcasted_iota(jnp.int32, (rows, n_tokens), 0)
        last = lax.axis_index("section") == lax.axis_size("section") - 1
        for offset, begin, end in ((0, 0, split), (capacity, split, columns)):
            total = jnp.zeros((n_tokens, end - begin), F32)
            for which, ref in enumerate(merged_refs):
                pick = jnp.zeros((rows, n_tokens), F32)
                for k in range(chosen):
                    target = jnp.where(relative[k : k + 1] == which, slot_rows[k], -2 * rows)
                    pick = pick + (row == target + offset).astype(F32)
                total = total + dot(pick.astype(BF16), ref[:, : end - begin], 0, 0)
            out_ref[:, begin:end] = jnp.where(last, 0.0, total).astype(BF16)

    return call(
        body,
        jax.ShapeDtypeStruct((n_tokens, columns), BF16),
        2 * 2 * n_tokens * columns * rows * len(merged),
        rows * columns * 2 * len(merged) + n_tokens * columns * 2,
    )(routes, *merged)


def per_device(token_grads, routing, gate_weights, layer_inputs, w_gate, w_up, w_down):
    n_groups = lax.axis_size("expert")
    n_sections = lax.axis_size("section")
    n_replicas = lax.axis_size("replica")
    n_experts = n_groups // SHARES
    grad_rows, inputs = token_grads[0], layer_inputs[0]
    routes, weights = routing[0].T, gate_weights[0].T
    gate_cols, up_cols, down_cols = w_gate[0], w_up[0], w_down[0]
    chosen, n_tokens = routes.shape
    columns = inputs.shape[1]
    width = gate_cols.shape[1]
    capacity = min(n_tokens, 17 * n_tokens * chosen // (16 * n_experts))
    split = round_up(columns // 2, 128)

    def partner(value, step):
        return lax.ppermute(value, "expert", [(j, j ^ step) for j in range(n_groups)])

    def across(j, which):
        expert, share = j // SHARES, j % SHARES
        return (expert + which) % n_experts * SHARES + (share ^ (2 if which else 0))

    def crossing(value, which):
        return lax.ppermute(
            value, "expert", [(j, across(j, which)) for j in range(n_groups)]
        )

    def homeward(value, which):
        pairs = [
            (s * n_groups + j, (s - 1) % n_sections * n_groups + across(j, -which))
            for s in range(n_sections)
            for j in range(n_groups)
        ]
        return lax.ppermute(value, ("section", "expert"), pairs)

    routes_next = lax.ppermute(
        routes, "section", [(s, (s - 1) % n_sections) for s in range(n_sections)]
    )
    halves = ((0, split), (split, columns))
    cuts = [((0, columns),)] + [halves] * (n_experts - 1)
    own = dispatch_blocks(routes, weights, grad_rows, inputs, cuts, capacity)
    staged = stage_weights(gate_cols, up_cols, down_cols)
    heads = [own[0]] + [
        [crossing(part, which) for part in own[which]]
        for which in range(1, n_experts)
    ]

    packed, slopes, merged = [], [], []
    for which in range(n_experts):
        head = heads[which]
        by_y = [partner(part, 1) for part in head]
        by_z = [partner(part, 2) for part in head]
        by_d = [partner(by_z[0], 1)]
        if which:
            by_d.append(partner(by_y[1], 2))
        part, rows_packed = partial_products(
            (head, by_y, by_z, by_d), staged, cuts[which], capacity
        )
        parts = [part]
        for turn in range(1, n_replicas):
            pairs = [(r, (r + turn) % n_replicas) for r in range(n_replicas)]
            parts.append(lax.ppermute(part, "replica", pairs))
        backs, slope = hidden_backward(parts, staged, capacity, split)
        packed.append(rows_packed)
        slopes.append(slope)
        total = backs[0].astype(F32)
        for step in range(1, SHARES):
            total = total + partner(backs[step], step).astype(F32)
        merged.append(homeward(total.astype(BF16), which))

    upstream = combine(routes_next, merged, n_experts, capacity, columns)
    grad_gate, grad_up, grad_down = weight_grads(packed, slopes, width)
    return (upstream[None], grad_gate[None], grad_up[None], grad_down[None])


def solution(mesh):
    placed = (
        P("section", "expert", "replica"),
        P("section", "expert", None),
        P("section", "expert", None),
        P("section", "expert", "replica"),
        P("section", "replica", "expert"),
        P("section", "replica", "expert"),
        P("section", "replica", "expert"),
    )

    return jax.shard_map(
        per_device,
        mesh=mesh,
        in_specs=placed,
        out_specs=(
            P("section", "expert", "replica"),
            P("section", "replica", "expert"),
            P("section", "replica", "expert"),
            P("section", "replica", "expert"),
        ),
        check_vma=False,
    )
```

```python
import functools

import jax
import jax.numpy as jnp
from jax import lax
from jax.experimental import pallas as pl
from jax.experimental.pallas import tpu as pltpu
from jax.sharding import PartitionSpec as P


SHARES = 4
F32 = jnp.float32
BF16 = jnp.bfloat16
VMEM_BYTES = 16 * 1024 * 1024


def round_up(value, multiple):
    return -(-value // multiple) * multiple


def call(body, out_shape, flops, n_bytes, scratch=(), in_specs=None):
    placed = {} if in_specs is None else {"in_specs": in_specs}
    return functools.partial(
        pl.pallas_call,
        out_shape=out_shape,
        scratch_shapes=list(scratch),
        **placed,
        compiler_params=pltpu.CompilerParams(vmem_limit_bytes=VMEM_BYTES),
        cost_estimate=pl.CostEstimate(flops=flops, bytes_accessed=n_bytes, transcendentals=0),
    )(body)


def in_hbm(value):
    return pltpu.with_memory_space_constraint(value, pltpu.HBM)


def dot(left, right, left_dim=1, right_dim=0):
    return lax.dot_general(
        left, right, (((left_dim,), (right_dim,)), ((), ())), preferred_element_type=F32
    )


def slots(routes, n_experts):
    chosen, n_tokens = routes.shape
    shift = lax.axis_index("expert") // SHARES
    relative = routes - shift
    relative = jnp.where(relative < 0, relative + n_experts, relative)
    experts = lax.broadcasted_iota(jnp.int32, (round_up(n_experts, 8), n_tokens), 0)
    named = [relative[k : k + 1] == experts for k in range(chosen)]
    count = sum(one.astype(F32) for one in named)
    earlier = (
        lax.broadcasted_iota(jnp.int32, (n_tokens, n_tokens), 0)
        < lax.broadcasted_iota(jnp.int32, (n_tokens, n_tokens), 1)
    ).astype(BF16)
    before = dot(count.astype(BF16), earlier)
    slot_rows = []
    for k in range(chosen):
        rank = jnp.sum(jnp.where(named[k], before, 0.0), axis=0, keepdims=True).astype(jnp.int32)
        for other in range(k):
            rank = rank + (relative[other : other + 1] == relative[k : k + 1]).astype(jnp.int32)
        slot_rows.append(rank)
    return relative, slot_rows


def dispatch_blocks(routes, weights, grad_rows, inputs, cuts, capacity):
    n_experts = len(cuts)
    chosen, n_tokens = routes.shape
    columns = inputs.shape[1]
    rows = round_up(2 * capacity, 8)
    order = list(range(1, n_experts)) + [0]

    operands = (routes, weights, inputs, grad_rows)
    first = [sum(len(one) for one in cuts[:which]) for which in range(n_experts)]
    n_outs = first[-1] + len(cuts[-1])

    def body(*refs):
        out_refs = list(refs[len(operands) : len(operands) + n_outs])
        *held, sems = refs[len(operands) + n_outs :]
        routes_ref, weights_ref, inputs_ref, grads_ref = held
        copies = [
            pltpu.make_async_copy(source, target, sems.at[i])
            for i, (source, target) in enumerate(zip(refs, held))
        ]
        for copy in copies:
            copy.start()
        copies[0].wait()
        relative, slot_rows = slots(routes_ref[...], n_experts)
        row = lax.broadcasted_iota(jnp.int32, (rows, n_tokens), 0)
        for copy in copies[1:]:
            copy.wait()
        for which in order:
            pick_input = jnp.zeros((rows, n_tokens), F32)
            pick_grad = jnp.zeros((rows, n_tokens), F32)
            scale = jnp.zeros((rows, n_tokens), F32)
            for k in range(chosen):
                target = jnp.where(relative[k : k + 1] == which, slot_rows[k], -2 * rows)
                pick_input = pick_input + (row == target).astype(F32)
                hit = (row == target + capacity).astype(F32)
                pick_grad = pick_grad + hit
                scale = scale + hit * weights_ref[k : k + 1, :]
            scale = jnp.sum(scale, axis=1, keepdims=True)
            pick_input = pick_input.astype(BF16)
            pick_grad = pick_grad.astype(BF16)
            for part, (begin, end) in enumerate(cuts[which]):
                block = dot(pick_input, inputs_ref[:, begin:end])
                block = block + dot(pick_grad, grads_ref[:, begin:end]) * scale
                out_refs[first[which] + part][...] = block.astype(BF16)

    outs = call(
        body,
        tuple(
            jax.ShapeDtypeStruct((rows, end - begin), BF16) for one in cuts for begin, end in one
        ),
        2 * 2 * n_experts * rows * n_tokens * columns,
        2 * n_tokens * columns * 2 + n_experts * rows * columns * 2,
        [pltpu.VMEM(value.shape, value.dtype) for value in operands]
        + [pltpu.SemaphoreType.DMA((len(operands),))],
        [pl.BlockSpec(memory_space=pltpu.HBM)] * len(operands),
    )(*(in_hbm(value) for value in operands))
    return [
        list(outs[first[which] : first[which] + len(cuts[which])]) for which in range(n_experts)
    ]


def stage_weights(gate_cols, up_cols, down_cols):
    columns, width = gate_cols.shape

    def body(gate_hbm, up_hbm, down_hbm, out_ref, sems):
        copies = [
            pltpu.make_async_copy(ref, out_ref.at[:, i * width : (i + 1) * width], sems.at[i])
            for i, ref in enumerate((gate_hbm, up_hbm, down_hbm))
        ]
        for copy in copies:
            copy.start()
        for copy in copies:
            copy.wait()

    return call(
        body,
        jax.ShapeDtypeStruct((columns, 3 * width), BF16),
        2 * columns * width * 256,
        6 * columns * width * 2,
        [pltpu.SemaphoreType.DMA((3,))],
        [pl.BlockSpec(memory_space=pltpu.HBM)] * 3,
    )(*(in_hbm(value) for value in (gate_cols, up_cols, down_cols)))


def partial_products(blocks, staged, capacity):
    rows = round_up(2 * capacity, 8)
    kept = round_up(capacity, 8)
    n_blocks = len(blocks)
    columns, width = staged.shape[0], staged.shape[1] // 3

    def body(*refs):
        block_refs = list(refs[: sum(len(block) for block in blocks)])
        staged_ref, out_ref, packed_ref = refs[len(block_refs) :]
        for i in range(n_blocks):
            begin = 0
            for _ in blocks[i]:
                ref = block_refs.pop(0)
                end = begin + ref.shape[1]
                packed_ref[i * rows : (i + 1) * rows, begin:end] = ref[...]
                begin = end
        packed = packed_ref[...]
        gate_up = dot(packed, staged_ref[:, : 2 * width])
        down = dot(packed, staged_ref[:, 2 * width :])
        for i in range(n_blocks):
            at = i * rows
            out_ref[i, :, : 2 * width] = gate_up[at : at + kept]
            out_ref[i, :capacity, 2 * width :] = down[at + capacity : at + 2 * capacity]
            if kept > capacity:
                out_ref[i, capacity:, 2 * width :] = jnp.zeros((kept - capacity, width), F32)

    return call(
        body,
        (
            jax.ShapeDtypeStruct((n_blocks, kept, 3 * width), F32),
            jax.ShapeDtypeStruct((n_blocks * rows, columns), BF16),
        ),
        2 * 3 * n_blocks * rows * columns * width,
        3 * columns * width * 2 + n_blocks * rows * columns * 4,
    )(*[part for block in blocks for part in block], staged)


def hidden_backward(partials, staged, capacity, split):
    n_blocks, kept, width3 = partials[0].shape
    columns, width = staged.shape[0], staged.shape[1] // 3
    rows = round_up(2 * capacity, 8)
    n_parts = len(partials)

    def body(*refs):
        part_refs = refs[:n_parts]
        staged_ref = refs[n_parts]
        back_refs = refs[n_parts + 1 : n_parts + 1 + n_blocks]
        slope_ref = refs[n_parts + 1 + n_blocks]
        valid = lax.broadcasted_iota(jnp.int32, (kept, width), 0) < capacity
        d_gates, d_ups = [], []
        slope_ref[...] = jnp.zeros(slope_ref.shape, BF16)
        for i in range(n_blocks):
            total = part_refs[0][i]
            for ref in part_refs[1:]:
                total = total + ref[i]
            gate = jnp.where(valid, total[:, :width], 0.0)
            up = jnp.where(valid, total[:, width : 2 * width], 0.0)
            grad_hidden = total[:, 2 * width :]
            sigmoid_gate = jax.nn.sigmoid(gate)
            activated = gate * sigmoid_gate
            hidden = (activated * up).astype(BF16)
            slope_term = sigmoid_gate * (1.0 + gate * (1.0 - sigmoid_gate))
            d_gate = (grad_hidden * up * slope_term).astype(BF16)
            d_up = (grad_hidden * activated).astype(BF16)
            at = i * rows
            slope_ref[at : at + capacity, :width] = d_gate[:capacity]
            slope_ref[at : at + capacity, width : 2 * width] = d_up[:capacity]
            slope_ref[at + capacity : at + 2 * capacity, 2 * width :] = hidden[:capacity]
            d_gates.append(d_gate)
            d_ups.append(d_up)
        slope = jnp.concatenate(
            [jnp.concatenate(d_gates, axis=0), jnp.concatenate(d_ups, axis=0)], axis=1
        )
        back = dot(slope, staged_ref[:, : 2 * width], 1, 1)
        for i in range(n_blocks):
            part = back[i * kept : i * kept + capacity].astype(BF16)
            back_refs[i][:capacity, :] = part[:, :split]
            back_refs[i][capacity : 2 * capacity, : columns - split] = part[:, split:]
            if columns < 2 * split:
                back_refs[i][capacity : 2 * capacity, columns - split :] = jnp.zeros(
                    (capacity, 2 * split - columns), BF16
                )
            if rows > 2 * capacity:
                back_refs[i][2 * capacity :, :] = jnp.zeros((rows - 2 * capacity, split), BF16)

    outs = call(
        body,
        tuple(jax.ShapeDtypeStruct((rows, split), BF16) for _ in range(n_blocks))
        + (jax.ShapeDtypeStruct((n_blocks * rows, width3), BF16),),
        2 * 2 * n_blocks * kept * columns * width,
        2 * columns * width * 2 + n_blocks * kept * columns * 2,
    )(*partials, staged)
    return outs[:n_blocks], outs[n_blocks]


def weight_grads(packed, slopes, width):
    columns = packed[0].shape[1]
    n_parts = len(packed)
    n_rows = sum(one.shape[0] for one in packed)

    def body(*refs):
        packed_refs = refs[:n_parts]
        slope_refs = refs[n_parts : 2 * n_parts]
        out_refs = refs[2 * n_parts :]
        total = dot(packed_refs[0][...], slope_refs[0][...], 0, 0)
        for left, right in zip(packed_refs[1:], slope_refs[1:]):
            total = total + dot(left[...], right[...], 0, 0)
        for i in range(3):
            out_refs[i][...] = total[:, i * width : (i + 1) * width].astype(BF16)

    return call(
        body,
        tuple(jax.ShapeDtypeStruct((columns, width), BF16) for _ in range(3)),
        2 * 3 * n_rows * columns * width,
        3 * columns * width * 2 + n_rows * columns * 2,
    )(*packed, *slopes)


def combine(routes, merged, n_experts, capacity, columns):
    chosen, n_tokens = routes.shape
    rows, split = merged[0][0].shape

    def body(routes_ref, *refs):
        refs, out_ref = list(refs[:-1]), refs[-1]
        relative, slot_rows = slots(routes_ref[...], n_experts)
        row = lax.broadcasted_iota(jnp.int32, (rows, n_tokens), 0)
        last = lax.axis_index("section") == lax.axis_size("section") - 1
        blocks = []
        for parts in merged:
            block = refs.pop(0)[...]
            if len(parts) > 1:
                block = block.astype(F32)
                for _ in parts[1:]:
                    block = block + refs.pop(0)[...].astype(F32)
            blocks.append(block.astype(BF16))
        for offset, begin, end in ((0, 0, split), (capacity, split, columns)):
            total = jnp.zeros((n_tokens, end - begin), F32)
            for which, block in enumerate(blocks):
                pick = jnp.zeros((rows, n_tokens), F32)
                for k in range(chosen):
                    target = jnp.where(relative[k : k + 1] == which, slot_rows[k], -2 * rows)
                    pick = pick + (row == target + offset).astype(F32)
                total = total + dot(pick.astype(BF16), block[:, : end - begin], 0, 0)
            out_ref[:, begin:end] = jnp.where(last, 0.0, total).astype(BF16)

    return call(
        body,
        jax.ShapeDtypeStruct((n_tokens, columns), BF16),
        2 * 2 * n_tokens * columns * rows * len(merged),
        rows * columns * 2 * len(merged) + n_tokens * columns * 2,
    )(routes, *[part for parts in merged for part in parts])


def per_device(token_grads, routing, gate_weights, layer_inputs, w_gate, w_up, w_down):
    n_groups = lax.axis_size("expert")
    n_sections = lax.axis_size("section")
    n_replicas = lax.axis_size("replica")
    n_experts = n_groups // SHARES
    grad_rows, inputs = token_grads[0], layer_inputs[0]
    routes, weights = routing[0].T, gate_weights[0].T
    gate_cols, up_cols, down_cols = w_gate[0], w_up[0], w_down[0]
    chosen, n_tokens = routes.shape
    columns = inputs.shape[1]
    width = gate_cols.shape[1]
    capacity = min(n_tokens, 17 * n_tokens * chosen // (16 * n_experts))
    split = round_up(columns // 2, 128)

    def partner(value, step):
        return lax.ppermute(value, "expert", [(j, j ^ step) for j in range(n_groups)])

    def across(j, which):
        expert, share = j // SHARES, j % SHARES
        return (expert + which) % n_experts * SHARES + (share ^ (2 if which else 0))

    def crossing(value, which):
        return lax.ppermute(
            value, "expert", [(j, across(j, which)) for j in range(n_groups)]
        )

    def homeward(value, target):
        pairs = [
            (s * n_groups + j, (s - 1) % n_sections * n_groups + target(j))
            for s in range(n_sections)
            for j in range(n_groups)
        ]
        return lax.ppermute(value, ("section", "expert"), pairs)

    routes_next = lax.ppermute(
        routes, "section", [(s, (s - 1) % n_sections) for s in range(n_sections)]
    )
    halves = ((0, split), (split, columns))
    cuts = [((0, columns),)] + [halves] * (n_experts - 1)
    own = dispatch_blocks(routes, weights, grad_rows, inputs, cuts, capacity)
    staged = stage_weights(gate_cols, up_cols, down_cols)
    heads = [own[0]] + [
        [crossing(part, which) for part in own[which]]
        for which in range(1, n_experts)
    ]

    shared = []
    for which, head in enumerate(heads):
        by_y = [partner(part, 1) for part in head]
        by_z = [partner(part, 2) for part in head]
        by_d = [partner(by_z[0], 1)]
        if which:
            by_d.append(partner(by_y[1], 2))
        shared.append((head, by_y, by_z, by_d))

    packed, slopes = [], []

    def returned(blocks):
        part, rows_packed = partial_products(blocks, staged, capacity)
        parts = [part]
        for turn in range(1, n_replicas):
            pairs = [(r, (r + turn) % n_replicas) for r in range(n_replicas)]
            parts.append(lax.ppermute(part, "replica", pairs))
        backs, slope = hidden_backward(parts, staged, capacity, split)
        packed.append(rows_packed)
        slopes.append(slope)
        return list(backs)

    backs = returned(shared[0][:3])
    backs_by_expert = [backs]
    for which in range(1, n_experts):
        if which == 1:
            backs = returned(shared[0][3:] + shared[1])
            backs_by_expert[0].append(backs.pop(0))
        else:
            backs = returned(shared[which])
        backs_by_expert.append(backs)
    if n_experts == 1:
        backs_by_expert[0] += returned(shared[0][3:])

    merged = [
        [
            homeward(back, lambda j, step=step: j ^ step)
            for step, back in enumerate(backs_by_expert[0])
        ]
    ]
    for which in range(1, n_experts):
        backs = backs_by_expert[which]
        total = backs[0].astype(F32)
        for step in range(1, SHARES):
            total = total + partner(backs[step], step).astype(F32)
        merged.append([homeward(total.astype(BF16), lambda j, which=which: across(j, -which))])

    upstream = combine(routes_next, merged, n_experts, capacity, columns)
    grad_gate, grad_up, grad_down = weight_grads(packed, slopes, width)
    return (upstream[None], grad_gate[None], grad_up[None], grad_down[None])


def solution(mesh):
    placed = (
        P("section", "expert", "replica"),
        P("section", "expert", None),
        P("section", "expert", None),
        P("section", "expert", "replica"),
        P("section", "replica", "expert"),
        P("section", "replica", "expert"),
        P("section", "replica", "expert"),
    )

    return jax.shard_map(
        per_device,
        mesh=mesh,
        in_specs=placed,
        out_specs=(
            P("section", "expert", "replica"),
            P("section", "replica", "expert"),
            P("section", "replica", "expert"),
            P("section", "replica", "expert"),
        ),
        check_vma=False,
    )
```

```python
import functools

import jax
import jax.numpy as jnp
from jax import lax
from jax.experimental import pallas as pl
from jax.experimental.pallas import tpu as pltpu
from jax.sharding import PartitionSpec as P


SHARES = 4
F32 = jnp.float32
BF16 = jnp.bfloat16
VMEM_BYTES = 16 * 1024 * 1024


def round_up(value, multiple):
    return -(-value // multiple) * multiple


def call(body, out_shape, flops, n_bytes, scratch=(), in_specs=None):
    placed = {} if in_specs is None else {"in_specs": in_specs}
    return functools.partial(
        pl.pallas_call,
        out_shape=out_shape,
        scratch_shapes=list(scratch),
        **placed,
        compiler_params=pltpu.CompilerParams(vmem_limit_bytes=VMEM_BYTES),
        cost_estimate=pl.CostEstimate(flops=flops, bytes_accessed=n_bytes, transcendentals=0),
    )(body)


def in_hbm(value):
    return pltpu.with_memory_space_constraint(value, pltpu.HBM)


def dot(left, right, left_dim=1, right_dim=0):
    return lax.dot_general(
        left, right, (((left_dim,), (right_dim,)), ((), ())), preferred_element_type=F32
    )


def slots(routes, n_experts):
    chosen, n_tokens = routes.shape
    shift = lax.axis_index("expert") // SHARES
    relative = routes - shift
    relative = jnp.where(relative < 0, relative + n_experts, relative)
    experts = lax.broadcasted_iota(jnp.int32, (round_up(n_experts, 8), n_tokens), 0)
    named = [relative[k : k + 1] == experts for k in range(chosen)]
    count = sum(one.astype(F32) for one in named)
    earlier = (
        lax.broadcasted_iota(jnp.int32, (n_tokens, n_tokens), 0)
        < lax.broadcasted_iota(jnp.int32, (n_tokens, n_tokens), 1)
    ).astype(BF16)
    before = dot(count.astype(BF16), earlier)
    slot_rows = []
    for k in range(chosen):
        rank = jnp.sum(jnp.where(named[k], before, 0.0), axis=0, keepdims=True).astype(jnp.int32)
        for other in range(k):
            rank = rank + (relative[other : other + 1] == relative[k : k + 1]).astype(jnp.int32)
        slot_rows.append(rank)
    return relative, slot_rows


def dispatch_blocks(routes, weights, grad_rows, inputs, cuts, capacity):
    n_experts = len(cuts)
    chosen, n_tokens = routes.shape
    columns = inputs.shape[1]
    rows = round_up(2 * capacity, 8)
    order = list(range(1, n_experts)) + [0]

    operands = (routes, weights, inputs, grad_rows)
    first = [sum(len(one) for one in cuts[:which]) for which in range(n_experts)]
    n_outs = first[-1] + len(cuts[-1])

    def body(*refs):
        out_refs = list(refs[len(operands) : len(operands) + n_outs])
        *held, sems = refs[len(operands) + n_outs :]
        routes_ref, weights_ref, inputs_ref, grads_ref = held
        copies = [
            pltpu.make_async_copy(source, target, sems.at[i])
            for i, (source, target) in enumerate(zip(refs, held))
        ]
        for copy in copies:
            copy.start()
        copies[0].wait()
        relative, slot_rows = slots(routes_ref[...], n_experts)
        row = lax.broadcasted_iota(jnp.int32, (rows, n_tokens), 0)
        for copy in copies[1:]:
            copy.wait()
        for which in order:
            pick_input = jnp.zeros((rows, n_tokens), F32)
            pick_grad = jnp.zeros((rows, n_tokens), F32)
            scale = jnp.zeros((rows, n_tokens), F32)
            for k in range(chosen):
                target = jnp.where(relative[k : k + 1] == which, slot_rows[k], -2 * rows)
                pick_input = pick_input + (row == target).astype(F32)
                hit = (row == target + capacity).astype(F32)
                pick_grad = pick_grad + hit
                scale = scale + hit * weights_ref[k : k + 1, :]
            scale = jnp.sum(scale, axis=1, keepdims=True)
            pick_input = pick_input.astype(BF16)
            pick_grad = pick_grad.astype(BF16)
            for part, (begin, end) in enumerate(cuts[which]):
                block = dot(pick_input, inputs_ref[:, begin:end])
                block = block + dot(pick_grad, grads_ref[:, begin:end]) * scale
                out_refs[first[which] + part][...] = block.astype(BF16)

    outs = call(
        body,
        tuple(
            jax.ShapeDtypeStruct((rows, end - begin), BF16) for one in cuts for begin, end in one
        ),
        2 * 2 * n_experts * rows * n_tokens * columns,
        2 * n_tokens * columns * 2 + n_experts * rows * columns * 2,
        [pltpu.VMEM(value.shape, value.dtype) for value in operands]
        + [pltpu.SemaphoreType.DMA((len(operands),))],
        [pl.BlockSpec(memory_space=pltpu.HBM)] * len(operands),
    )(*(in_hbm(value) for value in operands))
    return [
        list(outs[first[which] : first[which] + len(cuts[which])]) for which in range(n_experts)
    ]


def stage_weights(gate_cols, up_cols, down_cols):
    columns, width = gate_cols.shape

    def body(gate_hbm, up_hbm, down_hbm, out_ref, sems):
        copies = [
            pltpu.make_async_copy(ref, out_ref.at[:, i * width : (i + 1) * width], sems.at[i])
            for i, ref in enumerate((gate_hbm, up_hbm, down_hbm))
        ]
        for copy in copies:
            copy.start()
        for copy in copies:
            copy.wait()

    return call(
        body,
        jax.ShapeDtypeStruct((columns, 3 * width), BF16),
        2 * columns * width * 256,
        6 * columns * width * 2,
        [pltpu.SemaphoreType.DMA((3,))],
        [pl.BlockSpec(memory_space=pltpu.HBM)] * 3,
    )(*(in_hbm(value) for value in (gate_cols, up_cols, down_cols)))


def partial_products(blocks, staged, capacity):
    rows = round_up(2 * capacity, 8)
    kept = round_up(capacity, 8)
    n_blocks = len(blocks)
    columns, width = staged.shape[0], staged.shape[1] // 3

    def body(*refs):
        block_refs = list(refs[: sum(len(block) for block in blocks)])
        staged_ref, out_ref, packed_ref = refs[len(block_refs) :]
        for i in range(n_blocks):
            begin = 0
            for _ in blocks[i]:
                ref = block_refs.pop(0)
                end = begin + ref.shape[1]
                packed_ref[i * rows : (i + 1) * rows, begin:end] = ref[...]
                begin = end
        packed = packed_ref[...]
        gate_up = dot(packed, staged_ref[:, : 2 * width])
        down = dot(packed, staged_ref[:, 2 * width :])
        for i in range(n_blocks):
            at = i * rows
            out_ref[i, :, : 2 * width] = gate_up[at : at + kept]
            out_ref[i, :capacity, 2 * width :] = down[at + capacity : at + 2 * capacity]
            if kept > capacity:
                out_ref[i, capacity:, 2 * width :] = jnp.zeros((kept - capacity, width), F32)

    return call(
        body,
        (
            jax.ShapeDtypeStruct((n_blocks, kept, 3 * width), F32),
            jax.ShapeDtypeStruct((n_blocks * rows, columns), BF16),
        ),
        2 * 3 * n_blocks * rows * columns * width,
        3 * columns * width * 2 + n_blocks * rows * columns * 4,
    )(*[part for block in blocks for part in block], staged)


def hidden_backward(partials, staged, capacity, split):
    n_blocks, kept, width3 = partials[0].shape
    columns, width = staged.shape[0], staged.shape[1] // 3
    rows = round_up(2 * capacity, 8)
    n_parts = len(partials)

    def body(*refs):
        part_refs = refs[:n_parts]
        staged_ref = refs[n_parts]
        back_refs = refs[n_parts + 1 : n_parts + 1 + n_blocks]
        slope_ref = refs[n_parts + 1 + n_blocks]
        valid = lax.broadcasted_iota(jnp.int32, (kept, width), 0) < capacity
        d_gates, d_ups = [], []
        slope_ref[...] = jnp.zeros(slope_ref.shape, BF16)
        for i in range(n_blocks):
            total = part_refs[0][i]
            for ref in part_refs[1:]:
                total = total + ref[i]
            gate = jnp.where(valid, total[:, :width], 0.0)
            up = jnp.where(valid, total[:, width : 2 * width], 0.0)
            grad_hidden = total[:, 2 * width :]
            sigmoid_gate = jax.nn.sigmoid(gate)
            activated = gate * sigmoid_gate
            hidden = (activated * up).astype(BF16)
            slope_term = sigmoid_gate * (1.0 + gate * (1.0 - sigmoid_gate))
            d_gate = (grad_hidden * up * slope_term).astype(BF16)
            d_up = (grad_hidden * activated).astype(BF16)
            at = i * rows
            slope_ref[at : at + capacity, :width] = d_gate[:capacity]
            slope_ref[at : at + capacity, width : 2 * width] = d_up[:capacity]
            slope_ref[at + capacity : at + 2 * capacity, 2 * width :] = hidden[:capacity]
            d_gates.append(d_gate)
            d_ups.append(d_up)
        slope = jnp.concatenate(
            [jnp.concatenate(d_gates, axis=0), jnp.concatenate(d_ups, axis=0)], axis=1
        )
        back = dot(slope, staged_ref[:, : 2 * width], 1, 1)
        for i in range(n_blocks):
            part = back[i * kept : i * kept + capacity].astype(BF16)
            back_refs[i][:capacity, :] = part[:, :split]
            back_refs[i][capacity : 2 * capacity, : columns - split] = part[:, split:]
            if columns < 2 * split:
                back_refs[i][capacity : 2 * capacity, columns - split :] = jnp.zeros(
                    (capacity, 2 * split - columns), BF16
                )
            if rows > 2 * capacity:
                back_refs[i][2 * capacity :, :] = jnp.zeros((rows - 2 * capacity, split), BF16)

    outs = call(
        body,
        tuple(jax.ShapeDtypeStruct((rows, split), BF16) for _ in range(n_blocks))
        + (jax.ShapeDtypeStruct((n_blocks * rows, width3), BF16),),
        2 * 2 * n_blocks * kept * columns * width,
        2 * columns * width * 2 + n_blocks * kept * columns * 2,
    )(*partials, staged)
    return outs[:n_blocks], outs[n_blocks]


def weight_grads(packed, slopes, width):
    columns = packed[0].shape[1]
    n_parts = len(packed)
    n_rows = sum(one.shape[0] for one in packed)

    def body(*refs):
        packed_refs = refs[:n_parts]
        slope_refs = refs[n_parts : 2 * n_parts]
        out_refs = refs[2 * n_parts :]
        total = dot(packed_refs[0][...], slope_refs[0][...], 0, 0)
        for left, right in zip(packed_refs[1:], slope_refs[1:]):
            total = total + dot(left[...], right[...], 0, 0)
        for i in range(3):
            out_refs[i][...] = total[:, i * width : (i + 1) * width].astype(BF16)

    return call(
        body,
        tuple(jax.ShapeDtypeStruct((columns, width), BF16) for _ in range(3)),
        2 * 3 * n_rows * columns * width,
        3 * columns * width * 2 + n_rows * columns * 2,
    )(*packed, *slopes)


def combine_near(routes, backs, n_experts, capacity, columns):
    chosen, n_tokens = routes.shape
    rows, split = backs[0].shape
    lanes = round_up(rows, 128)

    def body(routes_ref, *refs):
        back_refs, (base_ref, pick_ref) = refs[:-2], refs[-2:]
        relative, slot_rows = slots(routes_ref[...], n_experts)
        row = lax.broadcasted_iota(jnp.int32, (lanes, n_tokens), 0)
        turned = (
            lax.broadcasted_iota(jnp.int32, (lanes, lanes), 0)
            == lax.broadcasted_iota(jnp.int32, (lanes, lanes), 1)
        ).astype(BF16)
        block = back_refs[0][...].astype(F32)
        for ref in back_refs[1:]:
            block = block + ref[...].astype(F32)
        block = block.astype(BF16)
        for which in range(n_experts):
            for half, (begin, end) in enumerate(((0, split), (split, columns))):
                pick = jnp.zeros((lanes, n_tokens), F32)
                for k in range(chosen):
                    target = jnp.where(relative[k : k + 1] == which, slot_rows[k], -2 * lanes)
                    pick = pick + (row == target + half * capacity).astype(F32)
                pick = dot(pick.astype(BF16), turned, 0, 0).astype(BF16)
                if which:
                    pick_ref[2 * (which - 1) + half] = pick
                else:
                    base_ref[:, begin:end] = dot(pick[:, :rows], block[:, : end - begin])

    return call(
        body,
        (
            jax.ShapeDtypeStruct((n_tokens, columns), F32),
            jax.ShapeDtypeStruct((max(1, 2 * (n_experts - 1)), n_tokens, lanes), BF16),
        ),
        2 * n_tokens * columns * rows,
        rows * columns * 2 * len(backs) + n_tokens * columns * 4,
    )(routes, *backs)


def combine_far(base, picks, merged, columns):
    n_tokens = base.shape[0]
    rows, split = merged[0].shape

    def body(base_ref, pick_ref, *refs):
        merged_refs, out_ref = refs[:-1], refs[-1]
        last = lax.axis_index("section") == lax.axis_size("section") - 1
        for half, (begin, end) in enumerate(((0, split), (split, columns))):
            total = base_ref[:, begin:end]
            for i, ref in enumerate(merged_refs):
                total = total + dot(pick_ref[2 * i + half][:, :rows], ref[:, : end - begin])
            out_ref[:, begin:end] = jnp.where(last, 0.0, total).astype(BF16)

    return call(
        body,
        jax.ShapeDtypeStruct((n_tokens, columns), BF16),
        2 * n_tokens * columns * rows * len(merged),
        rows * columns * 2 * len(merged) + n_tokens * columns * 6,
    )(base, picks, *merged)


def per_device(token_grads, routing, gate_weights, layer_inputs, w_gate, w_up, w_down):
    n_groups = lax.axis_size("expert")
    n_sections = lax.axis_size("section")
    n_replicas = lax.axis_size("replica")
    n_experts = n_groups // SHARES
    grad_rows, inputs = token_grads[0], layer_inputs[0]
    routes, weights = routing[0].T, gate_weights[0].T
    gate_cols, up_cols, down_cols = w_gate[0], w_up[0], w_down[0]
    chosen, n_tokens = routes.shape
    columns = inputs.shape[1]
    width = gate_cols.shape[1]
    capacity = min(n_tokens, 17 * n_tokens * chosen // (16 * n_experts))
    split = round_up(columns // 2, 128)

    def partner(value, step):
        return lax.ppermute(value, "expert", [(j, j ^ step) for j in range(n_groups)])

    def across(j, which):
        expert, share = j // SHARES, j % SHARES
        return (expert + which) % n_experts * SHARES + (share ^ (2 if which else 0))

    def crossing(value, which):
        return lax.ppermute(
            value, "expert", [(j, across(j, which)) for j in range(n_groups)]
        )

    def homeward(value, target):
        pairs = [
            (s * n_groups + j, (s - 1) % n_sections * n_groups + (target(j) if s else j))
            for s in range(n_sections)
            for j in range(n_groups)
        ]
        return lax.ppermute(value, ("section", "expert"), pairs)

    routes_next = lax.ppermute(
        routes, "section", [(s, (s - 1) % n_sections) for s in range(n_sections)]
    )
    lead = max(128, columns * 3 // 7 // 128 * 128)
    halves = ((0, lead), (lead, columns))
    cuts = [((0, columns),)] + [halves] * (n_experts - 1)
    own = dispatch_blocks(routes, weights, grad_rows, inputs, cuts, capacity)
    staged = stage_weights(gate_cols, up_cols, down_cols)
    heads = [own[0]] + [
        [crossing(part, which) for part in own[which]]
        for which in range(1, n_experts)
    ]

    shared = []
    for which, head in enumerate(heads):
        by_y = [partner(part, 1) for part in head]
        by_z = [partner(part, 2) for part in head]
        by_d = [partner(by_z[0], 1)]
        if which:
            by_d.append(partner(by_y[1], 2))
        shared.append((head, by_y, by_z, by_d))

    packed, slopes = [], []

    def returned(blocks):
        part, rows_packed = partial_products(blocks, staged, capacity)
        parts = [part]
        for turn in range(1, n_replicas):
            pairs = [(r, (r + turn) % n_replicas) for r in range(n_replicas)]
            parts.append(lax.ppermute(part, "replica", pairs))
        backs, slope = hidden_backward(parts, staged, capacity, split)
        packed.append(rows_packed)
        slopes.append(slope)
        return list(backs)

    early = SHARES - 1
    chunks = [returned(one[:early]) for one in shared[:2]]
    diagonals = returned([block for one in shared[:2] for block in one[early:]])
    chunks = [chunk + [diagonals[i]] for i, chunk in enumerate(chunks)]
    chunks += [returned(one) for one in shared[2:]]

    near = [homeward(back, lambda j, step=step: j ^ step) for step, back in enumerate(chunks[0])]
    merged = []
    for which in range(1, n_experts):
        backs = chunks[which]
        total = backs[0].astype(F32)
        for step in range(1, SHARES):
            total = total + partner(backs[step], step).astype(F32)
        merged.append(homeward(total.astype(BF16), lambda j, which=which: across(j, -which)))

    base, picks = combine_near(routes_next, near, n_experts, capacity, columns)
    upstream = combine_far(base, picks, merged, columns)
    grad_gate, grad_up, grad_down = weight_grads(packed, slopes, width)
    return (upstream[None], grad_gate[None], grad_up[None], grad_down[None])


def solution(mesh):
    placed = (
        P("section", "expert", "replica"),
        P("section", "expert", None),
        P("section", "expert", None),
        P("section", "expert", "replica"),
        P("section", "replica", "expert"),
        P("section", "replica", "expert"),
        P("section", "replica", "expert"),
    )

    return jax.shard_map(
        per_device,
        mesh=mesh,
        in_specs=placed,
        out_specs=(
            P("section", "expert", "replica"),
            P("section", "replica", "expert"),
            P("section", "replica", "expert"),
            P("section", "replica", "expert"),
        ),
        check_vma=False,
    )
```

```python
import functools

import jax
import jax.numpy as jnp
from jax import lax
from jax.experimental import pallas as pl
from jax.experimental.pallas import tpu as pltpu
from jax.sharding import PartitionSpec as P


SHARES = 4
F32 = jnp.float32
BF16 = jnp.bfloat16
VMEM_BYTES = 16 * 1024 * 1024


def round_up(value, multiple):
    return -(-value // multiple) * multiple


def call(body, out_shape, flops, n_bytes, scratch=(), in_specs=None, out_specs=None):
    placed = {} if in_specs is None else {"in_specs": in_specs}
    if out_specs is not None:
        placed["out_specs"] = out_specs
    return functools.partial(
        pl.pallas_call,
        out_shape=out_shape,
        scratch_shapes=list(scratch),
        **placed,
        compiler_params=pltpu.CompilerParams(vmem_limit_bytes=VMEM_BYTES),
        cost_estimate=pl.CostEstimate(flops=flops, bytes_accessed=n_bytes, transcendentals=0),
    )(body)


def in_hbm(value):
    return pltpu.with_memory_space_constraint(value, pltpu.HBM)


def dot(left, right, left_dim=1, right_dim=0):
    return lax.dot_general(
        left, right, (((left_dim,), (right_dim,)), ((), ())), preferred_element_type=F32
    )


def slots(routes, n_experts):
    chosen, n_tokens = routes.shape
    shift = lax.axis_index("expert") // SHARES
    relative = routes - shift
    relative = jnp.where(relative < 0, relative + n_experts, relative)
    experts = lax.broadcasted_iota(jnp.int32, (round_up(n_experts, 8), n_tokens), 0)
    named = [relative[k : k + 1] == experts for k in range(chosen)]
    count = sum(one.astype(F32) for one in named)
    earlier = (
        lax.broadcasted_iota(jnp.int32, (n_tokens, n_tokens), 0)
        < lax.broadcasted_iota(jnp.int32, (n_tokens, n_tokens), 1)
    ).astype(BF16)
    before = dot(count.astype(BF16), earlier)
    slot_rows = []
    for k in range(chosen):
        rank = jnp.sum(jnp.where(named[k], before, 0.0), axis=0, keepdims=True).astype(jnp.int32)
        for other in range(k):
            rank = rank + (relative[other : other + 1] == relative[k : k + 1]).astype(jnp.int32)
        slot_rows.append(rank)
    return relative, slot_rows


def dispatch_blocks(routes, weights, grad_rows, inputs, cuts, capacity):
    n_experts = len(cuts)
    chosen, n_tokens = routes.shape
    columns = inputs.shape[1]
    rows = round_up(2 * capacity, 8)
    order = list(range(1, n_experts)) + [0]

    operands = (routes, weights, inputs, grad_rows)
    first = [sum(len(one) for one in cuts[:which]) for which in range(n_experts)]
    n_outs = first[-1] + len(cuts[-1])

    def body(*refs):
        out_refs = list(refs[len(operands) : len(operands) + n_outs])
        *held, sems = refs[len(operands) + n_outs :]
        routes_ref, weights_ref, inputs_ref, grads_ref = held
        copies = [
            pltpu.make_async_copy(source, target, sems.at[i])
            for i, (source, target) in enumerate(zip(refs, held))
        ]
        for copy in copies:
            copy.start()
        copies[0].wait()
        relative, slot_rows = slots(routes_ref[...], n_experts)
        row = lax.broadcasted_iota(jnp.int32, (rows, n_tokens), 0)
        for copy in copies[1:]:
            copy.wait()
        for which in order:
            pick_input = jnp.zeros((rows, n_tokens), F32)
            pick_grad = jnp.zeros((rows, n_tokens), F32)
            scale = jnp.zeros((rows, n_tokens), F32)
            for k in range(chosen):
                target = jnp.where(relative[k : k + 1] == which, slot_rows[k], -2 * rows)
                pick_input = pick_input + (row == target).astype(F32)
                hit = (row == target + capacity).astype(F32)
                pick_grad = pick_grad + hit
                scale = scale + hit * weights_ref[k : k + 1, :]
            scale = jnp.sum(scale, axis=1, keepdims=True)
            pick_input = pick_input.astype(BF16)
            pick_grad = pick_grad.astype(BF16)
            for part, (begin, end) in enumerate(cuts[which]):
                block = dot(pick_input, inputs_ref[:, begin:end])
                block = block + dot(pick_grad, grads_ref[:, begin:end]) * scale
                out_refs[first[which] + part][...] = block.astype(BF16)

    outs = call(
        body,
        tuple(
            jax.ShapeDtypeStruct((rows, end - begin), BF16) for one in cuts for begin, end in one
        ),
        2 * 2 * n_experts * rows * n_tokens * columns,
        2 * n_tokens * columns * 2 + n_experts * rows * columns * 2,
        [pltpu.VMEM(value.shape, value.dtype) for value in operands]
        + [pltpu.SemaphoreType.DMA((len(operands),))],
        [pl.BlockSpec(memory_space=pltpu.HBM)] * len(operands),
    )(*(in_hbm(value) for value in operands))
    return [
        list(outs[first[which] : first[which] + len(cuts[which])]) for which in range(n_experts)
    ]


def stage_weights(gate_cols, up_cols, down_cols):
    columns, width = gate_cols.shape

    def body(gate_hbm, up_hbm, down_hbm, out_ref, sems):
        copies = [
            pltpu.make_async_copy(ref, out_ref.at[:, i * width : (i + 1) * width], sems.at[i])
            for i, ref in enumerate((gate_hbm, up_hbm, down_hbm))
        ]
        for copy in copies:
            copy.start()
        for copy in copies:
            copy.wait()

    return call(
        body,
        jax.ShapeDtypeStruct((columns, 3 * width), BF16),
        2 * columns * width * 256,
        6 * columns * width * 2,
        [pltpu.SemaphoreType.DMA((3,))],
        [pl.BlockSpec(memory_space=pltpu.HBM)] * 3,
    )(*(in_hbm(value) for value in (gate_cols, up_cols, down_cols)))


def partial_products(blocks, staged, capacity):
    rows = round_up(2 * capacity, 8)
    kept = round_up(capacity, 8)
    n_blocks = len(blocks)
    columns, width = staged.shape[0], staged.shape[1] // 3

    def body(*refs):
        block_refs = list(refs[: sum(len(block) for block in blocks)])
        staged_ref, out_ref, packed_ref, inputs_ref = refs[len(block_refs) :]
        for i in range(n_blocks):
            begin = 0
            for _ in blocks[i]:
                ref = block_refs.pop(0)
                end = begin + ref.shape[1]
                packed_ref[i * rows : (i + 1) * rows, begin:end] = ref[...]
                begin = end
        for i in range(n_blocks):
            at = i * rows
            inputs_ref[i * kept : (i + 1) * kept] = packed_ref[at : at + kept]
        gate_up = dot(inputs_ref[...], staged_ref[:, : 2 * width])
        down = dot(packed_ref[...], staged_ref[:, 2 * width :])
        for i in range(n_blocks):
            at = i * rows
            out_ref[i, :, : 2 * width] = gate_up[i * kept : (i + 1) * kept]
            out_ref[i, :capacity, 2 * width :] = down[at + capacity : at + 2 * capacity]
            if kept > capacity:
                out_ref[i, capacity:, 2 * width :] = jnp.zeros((kept - capacity, width), F32)

    return call(
        body,
        (
            jax.ShapeDtypeStruct((n_blocks, kept, 3 * width), F32),
            jax.ShapeDtypeStruct((n_blocks * rows, columns), BF16),
        ),
        2 * 3 * n_blocks * rows * columns * width,
        3 * columns * width * 2 + n_blocks * rows * columns * 4,
        [pltpu.VMEM((n_blocks * kept, columns), BF16)],
    )(*[part for block in blocks for part in block], staged)


def hidden_backward(partials, staged, capacity, split):
    n_blocks, kept, width3 = partials[0].shape
    columns, width = staged.shape[0], staged.shape[1] // 3
    rows = round_up(2 * capacity, 8)
    n_parts = len(partials)

    def body(*refs):
        part_refs = refs[:n_parts]
        staged_ref = refs[n_parts]
        back_refs = refs[n_parts + 1 : n_parts + 1 + n_blocks]
        slope_ref = refs[n_parts + 1 + n_blocks]
        valid = lax.broadcasted_iota(jnp.int32, (kept, width), 0) < capacity
        d_gates, d_ups = [], []
        slope_ref[...] = jnp.zeros(slope_ref.shape, BF16)
        for i in range(n_blocks):
            total = part_refs[0][i]
            for ref in part_refs[1:]:
                total = total + ref[i]
            gate = jnp.where(valid, total[:, :width], 0.0)
            up = jnp.where(valid, total[:, width : 2 * width], 0.0)
            grad_hidden = total[:, 2 * width :]
            sigmoid_gate = jax.nn.sigmoid(gate)
            activated = gate * sigmoid_gate
            hidden = (activated * up).astype(BF16)
            slope_term = sigmoid_gate * (1.0 + gate * (1.0 - sigmoid_gate))
            d_gate = (grad_hidden * up * slope_term).astype(BF16)
            d_up = (grad_hidden * activated).astype(BF16)
            at = i * rows
            slope_ref[at : at + capacity, :width] = d_gate[:capacity]
            slope_ref[at : at + capacity, width : 2 * width] = d_up[:capacity]
            slope_ref[at + capacity : at + 2 * capacity, 2 * width :] = hidden[:capacity]
            d_gates.append(d_gate)
            d_ups.append(d_up)
        slope = jnp.concatenate(
            [jnp.concatenate(d_gates, axis=0), jnp.concatenate(d_ups, axis=0)], axis=1
        )
        back = dot(slope, staged_ref[:, : 2 * width], 1, 1)
        for i in range(n_blocks):
            part = back[i * kept : i * kept + capacity].astype(BF16)
            back_refs[i][:capacity, :] = part[:, :split]
            back_refs[i][capacity : 2 * capacity, : columns - split] = part[:, split:]
            if columns < 2 * split:
                back_refs[i][capacity : 2 * capacity, columns - split :] = jnp.zeros(
                    (capacity, 2 * split - columns), BF16
                )
            if rows > 2 * capacity:
                back_refs[i][2 * capacity :, :] = jnp.zeros((rows - 2 * capacity, split), BF16)

    outs = call(
        body,
        tuple(jax.ShapeDtypeStruct((rows, split), BF16) for _ in range(n_blocks))
        + (jax.ShapeDtypeStruct((n_blocks * rows, width3), BF16),),
        2 * 2 * n_blocks * kept * columns * width,
        2 * columns * width * 2 + n_blocks * kept * columns * 2,
    )(*partials, staged)
    return outs[:n_blocks], outs[n_blocks]


def weight_grads(packed, slopes, width, first, last):
    columns = packed[0].shape[1]
    n_parts = len(packed)
    n_rows = sum(one.shape[0] for one in packed)

    def body(*refs):
        packed_refs = refs[:n_parts]
        slope_refs = refs[n_parts : 2 * n_parts]
        out_refs = refs[2 * n_parts :]
        begin, end = first * width, last * width
        total = dot(packed_refs[0][...], slope_refs[0][:, begin:end], 0, 0)
        for left, right in zip(packed_refs[1:], slope_refs[1:]):
            total = total + dot(left[...], right[:, begin:end], 0, 0)
        for i in range(last - first):
            out_refs[i][...] = total[:, i * width : (i + 1) * width].astype(BF16)

    return call(
        body,
        tuple(jax.ShapeDtypeStruct((columns, width), BF16) for _ in range(last - first)),
        2 * (last - first) * n_rows * columns * width,
        (last - first) * columns * width * 2 + n_rows * columns * 2,
    )(*packed, *slopes)


def combine_near(routes, backs, n_experts, capacity, columns):
    chosen, n_tokens = routes.shape
    rows, split = backs[0].shape
    lanes = round_up(rows, 128)

    def body(routes_ref, *refs):
        back_refs, (base_ref, pick_ref) = refs[:-2], refs[-2:]
        relative, slot_rows = slots(routes_ref[...], n_experts)
        row = lax.broadcasted_iota(jnp.int32, (lanes, n_tokens), 0)
        turned = (
            lax.broadcasted_iota(jnp.int32, (lanes, lanes), 0)
            == lax.broadcasted_iota(jnp.int32, (lanes, lanes), 1)
        ).astype(BF16)
        block = back_refs[0][...].astype(F32)
        for ref in back_refs[1:]:
            block = block + ref[...].astype(F32)
        block = block.astype(BF16)
        for which in range(n_experts):
            for half, (begin, end) in enumerate(((0, split), (split, columns))):
                pick = jnp.zeros((lanes, n_tokens), F32)
                for k in range(chosen):
                    target = jnp.where(relative[k : k + 1] == which, slot_rows[k], -2 * lanes)
                    pick = pick + (row == target + half * capacity).astype(F32)
                pick = dot(pick.astype(BF16), turned, 0, 0).astype(BF16)
                if which:
                    pick_ref[2 * (which - 1) + half] = pick
                else:
                    base_ref[:, begin:end] = dot(pick[:, :rows], block[:, : end - begin])

    return call(
        body,
        (
            jax.ShapeDtypeStruct((n_tokens, columns), F32),
            jax.ShapeDtypeStruct((max(1, 2 * (n_experts - 1)), n_tokens, lanes), BF16),
        ),
        2 * n_tokens * columns * rows,
        rows * columns * 2 * len(backs) + n_tokens * columns * 4,
    )(routes, *backs)


def combine_far(base, picks, merged, columns):
    n_tokens = base.shape[0]
    rows, split = merged[0].shape

    def body(base_ref, pick_ref, *refs):
        merged_refs, (out_hbm, held_ref, sems) = refs[:-3], refs[-3:]
        last = lax.axis_index("section") == lax.axis_size("section") - 1
        copies = []
        for half, (begin, end) in enumerate(((0, split), (split, columns))):
            total = base_ref[:, begin:end]
            for i, ref in enumerate(merged_refs):
                total = total + dot(pick_ref[2 * i + half][:, :rows], ref[:, : end - begin])
            held_ref[:, begin:end] = jnp.where(last, 0.0, total).astype(BF16)
            copies.append(
                pltpu.make_async_copy(
                    held_ref.at[:, begin:end], out_hbm.at[:, begin:end], sems.at[half]
                )
            )
            copies[-1].start()
        for copy in copies:
            copy.wait()

    return call(
        body,
        jax.ShapeDtypeStruct((n_tokens, columns), BF16),
        2 * n_tokens * columns * rows * len(merged),
        rows * columns * 2 * len(merged) + n_tokens * columns * 6,
        [pltpu.VMEM((n_tokens, columns), BF16), pltpu.SemaphoreType.DMA((2,))],
        out_specs=pl.BlockSpec(memory_space=pltpu.HBM),
    )(base, picks, *merged)


def per_device(token_grads, routing, gate_weights, layer_inputs, w_gate, w_up, w_down):
    n_groups = lax.axis_size("expert")
    n_sections = lax.axis_size("section")
    n_replicas = lax.axis_size("replica")
    n_experts = n_groups // SHARES
    grad_rows, inputs = token_grads[0], layer_inputs[0]
    routes, weights = routing[0].T, gate_weights[0].T
    gate_cols, up_cols, down_cols = w_gate[0], w_up[0], w_down[0]
    chosen, n_tokens = routes.shape
    columns = inputs.shape[1]
    width = gate_cols.shape[1]
    capacity = min(n_tokens, 17 * n_tokens * chosen // (16 * n_experts))
    split = round_up(columns // 2, 128)

    def partner(value, step):
        return lax.ppermute(value, "expert", [(j, j ^ step) for j in range(n_groups)])

    def across(j, which):
        expert, share = j // SHARES, j % SHARES
        return (expert + which) % n_experts * SHARES + (share ^ (2 if which else 0))

    def crossing(value, which):
        return lax.ppermute(
            value, "expert", [(j, across(j, which)) for j in range(n_groups)]
        )

    def homeward(value, target):
        pairs = [
            (s * n_groups + j, (s - 1) % n_sections * n_groups + (target(j) if s else j))
            for s in range(n_sections)
            for j in range(n_groups)
        ]
        return lax.ppermute(value, ("section", "expert"), pairs)

    routes_next = lax.ppermute(
        routes, "section", [(s, (s - 1) % n_sections) for s in range(n_sections)]
    )
    lead = max(128, columns * 3 // 7 // 128 * 128)
    halves = ((0, lead), (lead, columns))
    cuts = [((0, columns),)] + [halves] * (n_experts - 1)
    own = dispatch_blocks(routes, weights, grad_rows, inputs, cuts, capacity)
    staged = stage_weights(gate_cols, up_cols, down_cols)
    heads = [own[0]] + [
        [crossing(part, which) for part in own[which]]
        for which in range(1, n_experts)
    ]

    shared = []
    for which, head in enumerate(heads):
        by_y = [partner(part, 1) for part in head]
        by_z = [partner(part, 2) for part in head]
        by_d = [partner(by_z[0], 1)]
        if which:
            by_d.append(partner(by_y[1], 2))
        shared.append((head, by_y, by_z, by_d))

    packed, slopes = [], []

    def returned(blocks):
        part, rows_packed = partial_products(blocks, staged, capacity)
        parts = [part]
        for turn in range(1, n_replicas):
            pairs = [(r, (r + turn) % n_replicas) for r in range(n_replicas)]
            parts.append(lax.ppermute(part, "replica", pairs))
        backs, slope = hidden_backward(parts, staged, capacity, split)
        packed.append(rows_packed)
        slopes.append(slope)
        return list(backs)

    early = SHARES - 1
    chunks = [returned(one[:early]) for one in shared[:2]]
    diagonals = returned([block for one in shared[:2] for block in one[early:]])
    chunks = [chunk + [diagonals[i]] for i, chunk in enumerate(chunks)]
    chunks += [returned(one) for one in shared[2:]]

    near = [homeward(back, lambda j, step=step: j ^ step) for step, back in enumerate(chunks[0])]
    merged = []
    for which in range(1, n_experts):
        backs = chunks[which]
        total = backs[0].astype(F32)
        for step in range(1, SHARES):
            total = total + partner(backs[step], step).astype(F32)
        merged.append(homeward(total.astype(BF16), lambda j, which=which: across(j, -which)))

    base, picks = combine_near(routes_next, near, n_experts, capacity, columns)
    upstream = combine_far(base, picks, merged, columns)
    grad_gate, grad_up = weight_grads(packed, slopes, width, 0, 2)
    (grad_down,) = weight_grads(packed, slopes, width, 2, 3)
    return (upstream[None], grad_gate[None], grad_up[None], grad_down[None])


def solution(mesh):
    placed = (
        P("section", "expert", "replica"),
        P("section", "expert", None),
        P("section", "expert", None),
        P("section", "expert", "replica"),
        P("section", "replica", "expert"),
        P("section", "replica", "expert"),
        P("section", "replica", "expert"),
    )

    return jax.shard_map(
        per_device,
        mesh=mesh,
        in_specs=placed,
        out_specs=(
            P("section", "expert", "replica"),
            P("section", "replica", "expert"),
            P("section", "replica", "expert"),
            P("section", "replica", "expert"),
        ),
        check_vma=False,
    )
```
